32 devices in a mesh: cell: 8 (over y, x, core), gene: 4 (over z).
Axes of the slice: x: 2, y: 2, z: 4, core: 2. Of those that a mesh axis runs over, the one named last changes fastest.
Arguments:
- counts: int32 [3072, 8192], P('gene', 'cell'), may hold values from 0 to 11
- batch_id: int32 [8192], P('cell'), may hold values from 0 to 63
- live_cells: int32 [8], P('cell'), may hold values from 256 to 1024, as said below
- knot_bin: int32 [8192], P('cell'), may hold values from 0 to 14
- depth_frac: float32 [8192], P('cell'), may hold values from 0 to 1
- cell_covariates: float32 [16, 8192], P(None, 'cell'), may hold values from -3 to 3
- coefficients: float32 [3072, 32], P('gene'), may hold values from -1.2 to 1.2
- batch_effect: float32 [3072, 64], P('gene'), may hold values from -1.8 to 1.8
- factors: bfloat16 [8192, 64], P('cell'), may hold values from -4 to 4
- loadings: bfloat16 [3072, 64], P('gene'), may hold values from -0.19921875 to 0.19921875
Outputs:
- beta_step: float32 [3072, 32], P('gene')
- factor_step: float32 [8192, 64], P('cell')
- loading_score: float32 [3072, 64], P('gene')
The draws below stay inside these ranges and needn't reach their ends.
Inputs may be any that keep to these rules, and one draw needn't show every extreme that they name: `live_cells`: each index of the cell axis has its live cells in its first slots, at least 256 of them; some index is full in every draw.
All inputs are finite; a program needn't handle non-finite values.
Results may differ from the reference program's by a relative error of at most 0.0003.
Values sent between devices are 32-bit elements; how exact they have to be, the bound alone decides.
A program may use at most 64 MiB of HBM per device.

```python
import math
import jax
import jax.numpy as jnp
import numpy as np
from jax import lax

GENES = 3072
SPL = 16
COV = 16
FACTORS = 64
BATCHES = 64
CDEV = 1024
COVARS = 32
CELLS = 8192
NSHARD = 8
N_GENE = 4


def draw_live_cells(key, part):
    first_key, second_key = jax.random.split(jax.random.fold_in(key, 17))
    ladder = jax.random.randint(first_key, (NSHARD,), 0, 65)
    quarter = CDEV // 4
    live_count = quarter + (CDEV - quarter) * ladder * ladder // 4096
    chosen = jax.random.randint(second_key, (), 0, NSHARD)
    return jnp.where(jnp.arange(NSHARD, dtype=jnp.int32) == chosen, CDEV, live_count).astype(jnp.int32)


def set_ends(drawn, own_key, low, top_value):
    longest = drawn.shape.index(max(drawn.shape))
    spots = []
    for shift in (0, 1):
        where = [jax.random.randint(jax.random.fold_in(own_key, axis), (), 0, length) for axis, length in enumerate(drawn.shape)]
        where[longest] = (where[longest] + shift) % drawn.shape[longest]
        spots.append(tuple(where))
    return drawn.at[spots[0]].set(low).at[spots[1]].set(top_value)


def level_of(key, dims, cuts, low, largest):
    def one(position, shards_of):
        heights = jax.random.uniform(jax.random.fold_in(jax.random.fold_in(key, 6), position), (shards_of,), jnp.float32, low / len(cuts), largest / len(cuts))
        return jnp.repeat(jnp.exp(heights), dims[position] // shards_of).reshape((-1,) + (1,) * (len(dims) - position - 1))

    level = one(*cuts[0])
    for cut in cuts[1:]:
        level = level * one(*cut)
    return level


def rank_bounds(count, slope):
    loads = [(1 << 20) // math.isqrt(rank ** slope) + 1 for rank in range(1, count + 1)]
    scale = 1 + sum(loads) // (1 << 30)
    return np.cumsum(np.array([max(1, weight // scale) for weight in loads]))


def ranked_ids(stream_key, shape, amount, skew):
    listing = rank_bounds(amount, skew)
    lot = jax.random.randint(jax.random.fold_in(stream_key, 1), shape, 0, int(listing[amount - 1]))
    rank = jnp.searchsorted(jnp.asarray(listing, jnp.int32), lot, side="right")
    return jax.random.permutation(jax.random.fold_in(stream_key, 2), amount)[rank].astype(jnp.int32)


def scatter_about(rng, dims, deviation, most, cuts=(), kind=jnp.bfloat16):
    result = jax.random.normal(rng, dims, jnp.float32) * deviation
    if len(cuts) > 0:
        result = level_of(rng, dims, cuts, -0.22, 0.18) * result
    return jnp.clip(result, min=-most, max=most).astype(kind)


def setup_inputs(seed: int = 0) -> dict:
    splits = jax.random.split(jax.random.key(seed), 11)
    counts = set_ends(ranked_ids(splits[0], (GENES, CELLS), 12, 2), jax.random.fold_in(splits[0], 3), 0, 11).astype(jnp.int32)
    batch_id = set_ends(jax.random.randint(splits[1], (CELLS,), 0, BATCHES), jax.random.fold_in(splits[1], 1), 0, BATCHES - 1).astype(jnp.int32)
    live_cells = draw_live_cells(jax.random.fold_in(splits[10], 71), 0)
    knot_bin = set_ends(jax.random.randint(splits[3], (CELLS,), 0, SPL - 1), jax.random.fold_in(splits[3], 1), 0, (SPL - 1) - 1).astype(jnp.int32)
    depth_frac = jnp.clip(1.0 * jax.random.uniform(splits[4], (CELLS,), jnp.float32) ** level_of(splits[4], (CELLS,), ((0, 8),), -0.2, 0.2), 0.0, 1.0)
    cell_covariates = scatter_about(splits[5], (COV, CELLS), 0.5, 3.0, ((1, 8),), jnp.float32)
    coefficients = scatter_about(splits[6], (GENES, COVARS), 0.2, 1.2, ((0, 4),), jnp.float32)
    batch_effect = scatter_about(splits[7], (GENES, BATCHES), 0.3, 1.8, ((0, 4),), jnp.float32)
    factors = scatter_about(splits[8], (CELLS, FACTORS), 1.0, 4.0, ((0, 8),))
    loadings = scatter_about(splits[9], (GENES, FACTORS), 0.05, 0.19921875, ((0, 4),))
    return dict(counts=counts, batch_id=batch_id, live_cells=live_cells, knot_bin=knot_bin, depth_frac=depth_frac, cell_covariates=cell_covariates, coefficients=coefficients, batch_effect=batch_effect, factors=factors, loadings=loadings)


ridge_weight = 1.0

def design_rows(knot_bin, depth_frac, cell_covariates):
    levels = jnp.arange(SPL, dtype=jnp.int32)[:, None]
    fraction = depth_frac[None, :]
    hat_basis = jnp.where(levels == knot_bin[None, :], 1.0 - fraction, 0.0)
    hat_basis = hat_basis + jnp.where(levels == knot_bin[None, :] + 1, fraction, 0.0)
    return jnp.concatenate([hat_basis.astype(cell_covariates.dtype), cell_covariates], axis=0)

def newton_solve(gram_flat, score):
    columns = score.shape[-1]
    identity = jnp.eye(columns, dtype=gram_flat.dtype)
    system = gram_flat.reshape(-1, columns, columns) + ridge_weight * identity
    factor_lower = jnp.linalg.cholesky(system)
    middle = jax.scipy.linalg.solve_triangular(factor_lower, score[..., None], lower=True)
    return jax.scipy.linalg.solve_triangular(factor_lower, middle, lower=True, trans=1)[..., 0]

def reference(counts, batch_id, live_cells, knot_bin, depth_frac, cell_covariates, coefficients, batch_effect, factors, loadings):
    highest = lax.Precision.HIGHEST
    contract = (((1,), (1,)), ((), ()))
    totals = lax.optimization_barrier(jnp.sum(counts, axis=0)).astype(jnp.float32)
    offset = jnp.log((1.0 + totals) / GENES)
    positions = jnp.arange(CELLS, dtype=jnp.int32)
    live_mask = (positions % CDEV < live_cells[positions // CDEV]).astype(jnp.float32)
    design = design_rows(knot_bin, depth_frac, cell_covariates)
    columns = design.shape[0]
    pairs = (design[:, None, :] * design[None, :, :]).reshape(columns * columns, CELLS)
    onehot = (jnp.arange(BATCHES, dtype=jnp.int32)[:, None] == batch_id[None, :]).astype(jnp.float32)
    stacked = jnp.concatenate([design, onehot], axis=0)
    factors_wide = factors.astype(jnp.float32)
    gene_block = GENES // N_GENE

    def one_block(running, pieces):
        count_rows, coef_rows, shift_rows, load_rows = pieces
        observed = count_rows.astype(jnp.float32)
        linear = jnp.dot(jnp.concatenate([coef_rows, shift_rows], axis=1), stacked, precision=highest)
        latent = lax.dot_general(load_rows.astype(jnp.float32), factors.astype(jnp.float32), contract, preferred_element_type=jnp.float32)
        linear_pred = offset[None, :] + linear + latent
        expected = jnp.exp(linear_pred)
        weight = expected * live_mask
        residual = (observed - expected) * live_mask
        gram_part = lax.dot_general(weight, pairs, contract, precision=highest)
        score = lax.dot_general(residual, design, contract, precision=highest)
        beta_step = newton_solve(gram_part, score)
        expected_next = jnp.exp(linear_pred + jnp.dot(beta_step, design, precision=highest))
        weight_next = expected_next * live_mask
        residual_next = (observed - expected_next) * live_mask
        grad_load = jnp.dot(residual_next, factors_wide, precision=highest)
        curv_load = jnp.dot(weight_next, factors_wide * factors_wide, precision=highest)
        loads_wide = load_rows.astype(jnp.float32)
        back = (((0,), (0,)), ((), ()))
        grad_fact = running[0] + lax.dot_general(residual_next, loads_wide, back, precision=highest)
        curv_fact = running[1] + lax.dot_general(weight_next, loads_wide * loads_wide, back, precision=highest)
        return ((grad_fact, curv_fact), (beta_step, grad_load / jnp.sqrt(curv_load + 1.0)))
    pieces = (counts.reshape(N_GENE, gene_block, CELLS), coefficients.reshape(N_GENE, gene_block, columns), batch_effect.reshape(N_GENE, gene_block, BATCHES), loadings.reshape(N_GENE, gene_block, FACTORS))
    start = (jnp.zeros((CELLS, FACTORS), jnp.float32), jnp.zeros((CELLS, FACTORS), jnp.float32))
    sums, outputs = lax.scan(one_block, start, pieces)
    beta_step = outputs[0].reshape(GENES, columns)
    loading_score = outputs[1].reshape(GENES, FACTORS)
    factor_step = sums[0] / (sums[1] + 1.0)
    return (beta_step, factor_step, loading_score)
```

```python
import functools

import jax
import jax.numpy as jnp
from jax import lax
from jax.experimental import pallas as pl
from jax.experimental.pallas import tpu as pltpu
from jax.sharding import PartitionSpec as P

GENES = 3072
SPL = 16
BATCHES = 64


ridge_weight = 1.0


def design_rows(knot_bin, depth_frac, cell_covariates):
    levels = jnp.arange(SPL, dtype=jnp.int32)[:, None]
    fraction = depth_frac[None, :]
    hat_basis = jnp.where(levels == knot_bin[None, :], 1.0 - fraction, 0.0)
    hat_basis = hat_basis + jnp.where(levels == knot_bin[None, :] + 1, fraction, 0.0)
    return jnp.concatenate([hat_basis, cell_covariates], axis=0)


def newton_solve(gram_flat, score):
    columns = score.shape[-1]
    identity = jnp.eye(columns, dtype=gram_flat.dtype)
    system = gram_flat.reshape(-1, columns, columns) + ridge_weight * identity
    factor_lower = jnp.linalg.cholesky(system)
    middle = jax.scipy.linalg.solve_triangular(factor_lower, score[..., None], lower=True)
    return jax.scipy.linalg.solve_triangular(factor_lower, middle, lower=True, trans=1)[..., 0]


def local_plain(
    counts,
    batch_id,
    live_cells,
    knot_bin,
    depth_frac,
    cell_covariates,
    coefficients,
    batch_effect,
    factors,
    loadings,
):
    highest = lax.Precision.HIGHEST
    contract = (((1,), (1,)), ((), ()))
    observed = counts.astype(jnp.float32)
    totals = lax.psum(jnp.sum(observed, axis=0), "gene")
    offset = jnp.log((1.0 + totals) / GENES)
    slot_count = observed.shape[1]
    live_mask = (jnp.arange(slot_count, dtype=jnp.int32) < live_cells[0]).astype(jnp.float32)
    design = design_rows(knot_bin, depth_frac, cell_covariates)
    columns = design.shape[0]
    onehot = (jnp.arange(BATCHES, dtype=jnp.int32)[:, None] == batch_id[None, :]).astype(
        jnp.float32
    )
    stacked = jnp.concatenate([design, onehot], axis=0)
    linear = jnp.dot(
        jnp.concatenate([coefficients, batch_effect], axis=1), stacked, precision=highest
    )
    latent = lax.dot_general(loadings, factors, contract, preferred_element_type=jnp.float32)
    linear_pred = offset[None, :] + linear + latent
    expected = jnp.exp(linear_pred)
    weight = expected * live_mask
    residual = (observed - expected) * live_mask
    pairs = (design[:, None, :] * design[None, :, :]).reshape(columns * columns, slot_count)
    gram_part = lax.dot_general(weight, pairs, contract, precision=highest)
    score_part = lax.dot_general(residual, design, contract, precision=highest)
    gram_share, score_share = (
        lax.psum_scatter(gram_part, "cell", scatter_dimension=0, tiled=True),
        lax.psum_scatter(score_part, "cell", scatter_dimension=0, tiled=True),
    )
    step_share = newton_solve(gram_share, score_share)
    beta_step = lax.all_gather(step_share, "cell", axis=0, tiled=True)
    expected_next = jnp.exp(linear_pred + jnp.dot(beta_step, design, precision=highest))
    weight_next = expected_next * live_mask
    residual_next = (observed - expected_next) * live_mask
    factors_wide = factors.astype(jnp.float32)
    loads_wide = loadings.astype(jnp.float32)
    grad_load = jnp.dot(residual_next, factors_wide, precision=highest)
    curv_load = jnp.dot(weight_next, factors_wide * factors_wide, precision=highest)
    back = (((0,), (0,)), ((), ()))
    grad_fact = lax.dot_general(residual_next, loads_wide, back, precision=highest)
    curv_fact = lax.dot_general(weight_next, loads_wide * loads_wide, back, precision=highest)
    grad_load, curv_load = lax.psum((grad_load, curv_load), "cell")
    grad_fact, curv_fact = lax.psum((grad_fact, curv_fact), "gene")
    factor_step = grad_fact / (curv_fact + 1.0)
    loading_score = grad_load / jnp.sqrt(curv_load + 1.0)
    return (beta_step, factor_step, loading_score)


MESH = pl.DeviceIdType.MESH
F32, BF16 = jnp.float32, jnp.bfloat16
VM = pl.BlockSpec(memory_space=pltpu.VMEM)
ROWS_BY_ROWS = (((1,), (1,)), ((), ()))
ACROSS = (((1,), (0,)), ((), ()))
DOWN = (((0,), (0,)), ((), ()))
LIMIT = 60 * 1024 * 1024


def split(x):
    high = x.astype(BF16)
    return high, (x - high.astype(F32)).astype(BF16)


def mul(a, b, dims):
    return lax.dot_general(a, b, dims, preferred_element_type=F32)


def remote(src, dst, send, recv, where):
    return pltpu.make_async_remote_copy(
        src_ref=src, dst_ref=dst, send_sem=send, recv_sem=recv, device_id=where, device_id_type=MESH
    )


def meet_signal(groups):
    barrier = pltpu.get_barrier_semaphore()
    count = 0
    for axis, n in groups:
        me = lax.axis_index(axis)
        for d in range(1, n):
            pl.semaphore_signal(
                barrier, inc=1, device_id={axis: lax.rem(me + d, n)}, device_id_type=MESH
            )
        count += n - 1
    return lambda: pl.semaphore_wait(barrier, count)


def design_of(knot_ref, frac_ref, cov_ref):
    slots = knot_ref.shape[1]
    levels = lax.broadcasted_iota(jnp.int32, (SPL, slots), 0)
    knot, frac = knot_ref[...], frac_ref[...]
    hats = jnp.where(levels == knot, 1.0 - frac, 0.0)
    hats = hats + jnp.where(levels == knot + 1, frac, 0.0)
    return hats, cov_ref[...]


def build_pairs(hats, cov, pair_hi, pair_lo):
    slots = hats.shape[1]
    ncov = cov.shape[0]
    half = ncov // 2

    def put(at, block):
        high, low = split(block)
        pair_hi[at : at + block.shape[0]] = high
        pair_lo[at : at + block.shape[0]] = low

    at = 0
    for p in range(SPL):
        put(at, hats[p : p + 1] * cov)
        at += ncov
    for i in range(half):
        put(at, cov[i : i + 1] * cov)
        at += ncov
    for i in range(half, ncov, 2):
        put(
            at,
            jnp.concatenate(
                [cov[i : i + 1] * cov[half:], cov[i + 1 : i + 2] * cov[half:]], axis=0
            ),
        )
        at += ncov
    put(at, hats * hats)
    at += SPL
    later = jnp.concatenate([hats[1:], jnp.zeros((1, slots), F32)], axis=0)
    put(at, hats * later)
    at += SPL
    put(at, jnp.zeros((SPL + ncov, slots), F32))


def solve(g, x):
    half = SPL // 2
    cov_at, low_at, hat_at = SPL * SPL, SPL * SPL + half * SPL, SPL * SPL + half * SPL + half * half
    off_at, score_at = hat_at + SPL, hat_at + 2 * SPL
    spot = lax.broadcasted_iota(jnp.int32, (half, g.shape[1]), 0)

    def one(block, i):
        return block[i : i + 1]

    lo = {}
    hi = {}
    for i in range(SPL):
        unit = jnp.where(spot == i % half, ridge_weight, 0.0)
        if i < half:
            lo[i] = g[cov_at + i * SPL : cov_at + i * SPL + half] + unit
            hi[i] = g[cov_at + i * SPL + half : cov_at + (i + 1) * SPL]
        else:
            hi[i] = g[low_at + (i - half) * half : low_at + (i - half + 1) * half] + unit
    b_lo = g[score_at + SPL : score_at + SPL + half]
    b_hi = g[score_at + SPL + half : score_at + 2 * SPL]
    sums_lo, sums_hi = g[0:half], g[half:SPL]
    for p in range(1, SPL):
        sums_lo = sums_lo + g[p * SPL : p * SPL + half]
        sums_hi = sums_hi + g[p * SPL + half : (p + 1) * SPL]
    b_lo, b_hi = b_lo - sums_lo, b_hi - sums_hi
    pivot_inv, edge, side_lo, side_hi, rest = [], [], [], [], []
    for p in range(SPL):
        own = g[hat_at + p : hat_at + p + 1]
        after = g[off_at + p : off_at + p + 1]
        d = own + ridge_weight
        u_lo = g[p * SPL : p * SPL + half]
        u_hi = g[p * SPL + half : (p + 1) * SPL]
        b = g[score_at + p : score_at + p + 1] - own - after
        if p > 0:
            b = b - edge[-1]
            ratio = edge[-1] * pivot_inv[-1]
            d = d - ratio * edge[-1]
            u_lo = u_lo - ratio * side_lo[-1]
            u_hi = u_hi - ratio * side_hi[-1]
            b = b - ratio * rest[-1]
        inv = 1.0 / d
        pivot_inv.append(inv)
        edge.append(after)
        side_lo.append(u_lo)
        side_hi.append(u_hi)
        rest.append(b)
        scaled_lo, scaled_hi = u_lo * inv, u_hi * inv
        b_lo = b_lo - scaled_lo * b
        b_hi = b_hi - scaled_hi * b
        for i in range(SPL):
            if i < half:
                f = one(scaled_lo, i)
                lo[i] = lo[i] - f * u_lo
            else:
                f = one(scaled_hi, i - half)
            hi[i] = hi[i] - f * u_hi
    c_inv, c_rest = [], []
    for j in range(SPL):
        if j < half:
            inv = 1.0 / one(lo[j], j)
            b = one(b_lo, j)
            s_lo = lo[j] * inv
            b_lo = b_lo - s_lo * b
        else:
            inv = 1.0 / one(hi[j], j - half)
            b = one(b_hi, j - half)
        s_hi = hi[j] * inv
        b_hi = b_hi - s_hi * b
        c_inv.append(inv)
        c_rest.append(b)
        for i in range(j + 1, SPL):
            if i < half:
                f = one(s_lo, i)
                lo[i] = lo[i] - f * lo[j]
            else:
                f = one(s_hi, i - half)
            hi[i] = hi[i] - f * hi[j]
    for j in reversed(range(SPL)):
        found = c_rest[j] * c_inv[j]
        x[SPL + j : SPL + j + 1] = found
        for i in range(j):
            c_rest[i] = c_rest[i] - (one(hi[i], j - half) if j >= half else one(lo[i], j)) * found
    x_lo, x_hi = x[SPL : SPL + half], x[SPL + half : 2 * SPL]
    after = None
    for p in reversed(range(SPL)):
        gone = jnp.sum(side_lo[p] * x_lo + side_hi[p] * x_hi, axis=0, keepdims=True)
        b = rest[p] - gone
        if after is not None:
            b = b - edge[p] * after
        after = b * pivot_inv[p]
        x[p : p + 1] = after


def all_kernel(
    n, m, counts_hbm, batch_ref, live_ref, knot_ref, frac_ref, cov_ref, coef_ref, shift_ref,
    factors_ref, loads_ref, beta_ref, fs_ref, ls_ref,
    counts, lin, rhs, pair_hi, pair_lo, tally, f_all, l_all, extra, tot_out, tot_in, known_c, known_f,
    w_hi, w_lo, lhs_ref, g, g_pair, g_out, g_far, tall, turned, mine, theirs,
    gl, l_pair, l_out, l_far, my_l, their_l, gf, from_g, my_f, their_f,
    c_sem, t_send, t_recv, gp_send, gp_recv, gf_send, gf_recv, b_send, b_recv,
    lp_send, lp_recv, lf_send, lf_recv, ol_send, ol_recv, z_send, z_recv, of_send, of_recv,
):
    cell, gene = lax.axis_index("cell"), lax.axis_index("gene")
    core, chip = lax.rem(cell, 2), cell // 2
    chips = n // 2
    genes, slots = counts.shape
    block = genes // chips
    rows = genes // n
    latent = loads_ref.shape[0]
    span = slots // m
    arrive = meet_signal((("cell", n), ("gene", m)))
    loads_in = []
    for i in range(n):
        at = pl.ds(i * rows, rows)
        loads_in.append(pltpu.make_async_copy(counts_hbm.at[at], counts.at[at], c_sem.at[i]))
        loads_in[-1].start()
    part = None
    for i in range(n):
        loads_in[i].wait()
        piece = jnp.sum(counts[i * rows : (i + 1) * rows].reshape(rows // 8, 8, slots), axis=0)
        part = piece if part is None else part + piece
    tot_out[...] = jnp.sum(part, axis=0, keepdims=True).astype(F32)
    arrive()
    tot = []
    for d in range(1, m):
        tot.append(
            remote(
                tot_out, tot_in.at[d - 1], t_send.at[d - 1], t_recv.at[d - 1],
                {"gene": lax.rem(gene + d, m)},
            )
        )
        tot[-1].start()

    hats, cov = design_of(knot_ref, frac_ref, cov_ref)
    width = hats.shape[0] + cov.shape[0]
    design_hi, design_lo = split(jnp.concatenate([hats, cov], axis=0))
    hot = lax.broadcasted_iota(jnp.int32, (BATCHES, slots), 0) == batch_ref[...]
    hot = jnp.where(hot, 1.0, 0.0).astype(BF16)
    rhs[0:width] = design_hi
    rhs[width : 2 * width] = design_hi
    rhs[2 * width : 3 * width] = design_lo
    rhs[3 * width : 3 * width + BATCHES] = hot
    rhs[3 * width + BATCHES : 3 * width + 2 * BATCHES] = hot
    rhs[3 * width + 2 * BATCHES :] = factors_ref[...]
    coef_hi, coef_lo = split(coef_ref[...])
    shift_hi, shift_lo = split(shift_ref[...])
    lhs = jnp.concatenate([coef_hi, coef_lo, coef_hi, shift_hi, shift_lo, loads_ref[...]], axis=0)
    lin[...] = mul(lhs, rhs[...], DOWN)
    build_pairs(hats, cov, pair_hi, pair_lo)
    live = lax.broadcasted_iota(jnp.int32, (1, slots), 1) < live_ref[...]
    mask = jnp.where(live, 1.0, 0.0)
    mask_bf = mask.astype(BF16)
    tally[0:width] = design_hi * mask_bf
    tally[width : 2 * width] = design_lo * mask_bf
    factors_live = factors_ref[...].astype(F32) * mask
    tally[2 * width :] = factors_live.astype(BF16)
    f_hi, f_lo = split(factors_live * factors_live)
    f_all[0:latent] = factors_live.astype(BF16)
    f_all[latent : 2 * latent] = f_hi
    f_all[2 * latent :] = f_lo
    loads_wide = loads_ref[...].astype(F32)
    l_hi, l_lo = split(loads_wide * loads_wide)
    l_all[0:latent] = loads_ref[...]
    l_all[latent : 2 * latent] = l_hi
    l_all[2 * latent :] = l_lo
    counts_bf = counts[...].astype(F32).astype(BF16)
    known_c[...] = mul(counts_bf, tally[...], ROWS_BY_ROWS)
    known_f[...] = mul(l_all[0:latent], counts_bf, ACROSS) * mask

    total = tot_out[...]
    for d in range(1, m):
        tot[d - 1].wait()
        total = total + tot_in[d - 1]
    extra[0:1] = jnp.where(live, jnp.log((1.0 + total) / GENES), -1e30)

    places = [chips - 1 - chip, chip + 1 - 2 * lax.rem(chip, 2), lax.rem(chip + 2, chips), chip]

    def hand_on(j, mine_ref, pair_ref, copy, out_ref, far_ref, send, recv):
        copy.wait()
        if j == chips - 1:
            return None
        out_ref[j] = mine_ref[j, core] + pair_ref[j]
        far = remote(
            out_ref.at[j], far_ref.at[j], send.at[j], recv.at[j], {"cell": 2 * places[j] + core}
        )
        far.start()
        return far

    partner = cell + 1 - 2 * core
    wide = g.shape[3]
    pair, far = [], []
    for j in range(chips):
        at = pl.ds(pl.multiple_of(places[j] * block, block), block)
        linear = lin[at] + extra[0:1]
        lin[at] = linear
        high, low = split(jnp.exp(linear))
        both = mul(jnp.concatenate([high, low], axis=0), pair_hi[...], ROWS_BY_ROWS)
        gram = both[:block] + both[block:] + mul(high, pair_lo[...], ROWS_BY_ROWS)
        counted = known_c[at, 0:width] + known_c[at, width : 2 * width]
        g[j, :, :, : wide - width] = gram[:, : wide - width].reshape(2, rows, wide - width)
        g[j, :, :, wide - width :] = counted.reshape(2, rows, width)
        pair.append(
            remote(g.at[j, 1 - core], g_pair.at[j], gp_send.at[j], gp_recv.at[j], {"cell": partner})
        )
        pair[-1].start()
        if j > 0:
            far.append(
                hand_on(j - 1, g, g_pair, pair[j - 1], g_out, g_far, gf_send, gf_recv)
            )
    hand_on(chips - 1, g, g_pair, pair[-1], g_out, g_far, gf_send, gf_recv)
    total = g[chips - 1, core] + g_pair[chips - 1]
    for j in range(chips - 1):
        far[j].wait()
        total = total + g_far[j]
    tall[0:rows] = total
    if rows < 128:
        tall[rows:128] = jnp.zeros((128 - rows, wide), F32)
    turned[...] = tall[...].T
    solve(turned, mine)
    out = []
    for d in range(1, n):
        out.append(
            remote(
                mine, theirs.at[cell], b_send.at[d - 1], b_recv.at[d - 1],
                {"cell": lax.rem(cell + d, n)},
            )
        )
        out[-1].start()
    theirs[cell] = mine[...]
    for d in range(1, n):
        out[d - 1].wait()
    for o in range(n):
        beta_ref[:, o * rows : (o + 1) * rows] = theirs[o, :, :rows]
    beta_hi, beta_lo = split(beta_ref[...])
    lhs_ref[...] = jnp.concatenate([beta_hi, beta_lo, beta_hi], axis=0).astype(F32).T.astype(BF16)

    along = []
    for d in list(range(1, m)) + [0]:
        to = lax.rem(gene + d, m)
        cols = pl.ds(pl.multiple_of(to * span, span), span)
        delta = mul(lhs_ref[...], rhs[0 : 3 * width, cols], ACROSS)
        high, low = split(jnp.exp(lin[:, cols] + delta))
        w_hi[:, cols] = high
        w_lo[:, cols] = low
        first = mul(l_all[...], high, ACROSS)
        second = mul(l_all[0 : 2 * latent], low, ACROSS)
        gf[d, :latent] = known_f[:, cols] - first[:latent] - second[:latent]
        gf[d, latent:] = first[latent : 2 * latent] + first[2 * latent :] + second[latent:]
        if d > 0:
            along.append(
                remote(gf.at[d], from_g.at[d - 1], z_send.at[d - 1], z_recv.at[d - 1], {"gene": to})
            )
            along[-1].start()
    lpair, lfar = [], []
    for j in range(chips):
        at = pl.ds(pl.multiple_of(places[j] * block, block), block)
        first = mul(w_hi[at], f_all[...], ROWS_BY_ROWS)
        second = mul(w_lo[at], f_all[0 : 2 * latent], ROWS_BY_ROWS)
        grad = known_c[at, 2 * width :] - first[:, :latent] - second[:, :latent]
        curv = first[:, latent : 2 * latent] + first[:, 2 * latent :] + second[:, latent:]
        gl[j] = jnp.concatenate([grad, curv], axis=1).reshape(2, rows, 2 * latent)
        lpair.append(
            remote(gl.at[j, 1 - core], l_pair.at[j], lp_send.at[j], lp_recv.at[j], {"cell": partner})
        )
        lpair[-1].start()
        if j > 0:
            lfar.append(
                hand_on(j - 1, gl, l_pair, lpair[j - 1], l_out, l_far, lf_send, lf_recv)
            )
    hand_on(chips - 1, gl, l_pair, lpair[-1], l_out, l_far, lf_send, lf_recv)
    total = gl[chips - 1, core] + l_pair[chips - 1]
    for j in range(chips - 1):
        lfar[j].wait()
        total = total + l_far[j]
    if rows < 128:
        total = jnp.concatenate([total, jnp.zeros((128 - rows, 2 * latent), F32)], axis=0)
    total = total.T
    my_l[...] = total[:latent] / jnp.sqrt(total[latent:] + 1.0)
    out_l, out_f = [], []
    for d in range(1, n):
        out_l.append(
            remote(
                my_l, their_l.at[cell], ol_send.at[d - 1], ol_recv.at[d - 1],
                {"cell": lax.rem(cell + d, n)},
            )
        )
        out_l[-1].start()
    their_l[cell] = my_l[...]
    total = gf[0]
    for d in range(1, m):
        along[d - 1].wait()
        total = total + from_g[d - 1]
    my_f[...] = total[:latent] / (total[latent:] + 1.0)
    for d in range(1, m):
        out_f.append(
            remote(
                my_f, their_f.at[gene], of_send.at[d - 1], of_recv.at[d - 1],
                {"gene": lax.rem(gene + d, m)},
            )
        )
        out_f[-1].start()
    their_f[gene] = my_f[...]
    for d in range(1, n):
        out_l[d - 1].wait()
    for o in range(n):
        ls_ref[:, o * rows : (o + 1) * rows] = their_l[o, :, :rows]
    for d in range(1, m):
        out_f[d - 1].wait()
    for o in range(m):
        fs_ref[:, o * span : (o + 1) * span] = their_f[o]


def pass_on(*refs):
    count = len(refs) // 2
    for source, target in zip(refs[:count], refs[count:]):
        target[...] = source[...]


def local_fused(
    n, m, counts, batch_id, live_cells, knot_bin, depth_frac, cell_covariates, coefficients,
    batch_effect, factors, loadings,
):
    genes, slots = counts.shape
    rows, span, latent = genes // n, slots // m, factors.shape[1]
    ncov = cell_covariates.shape[0]
    width = SPL + ncov
    wide = SPL * ncov + ncov * ncov * 3 // 4 + 2 * SPL + width
    chips = n // 2
    dma = pltpu.SemaphoreType.DMA
    shape = jax.ShapeDtypeStruct
    vmem = pltpu.VMEM

    def params(**kw):
        return pltpu.CompilerParams(vmem_limit_bytes=LIMIT, **kw)

    knot, frac, batch = (v.reshape(1, slots) for v in (knot_bin, depth_frac, batch_id))
    shapes = (shape((width, genes), F32), shape((latent, slots), F32), shape((latent, genes), F32))
    found = pl.pallas_call(
        functools.partial(all_kernel, n, m),
        out_shape=shapes,
        in_specs=[pl.BlockSpec(memory_space=pl.ANY)] + [VM] * 9,
        out_specs=(VM, VM, VM),
        scratch_shapes=[
            vmem((genes, slots), jnp.int32),
            vmem((genes, slots), F32),
            vmem((3 * width + 2 * BATCHES + latent, slots), BF16),
            vmem((wide, slots), BF16),
            vmem((wide, slots), BF16),
            vmem((2 * width + latent, slots), BF16),
            vmem((3 * latent, slots), BF16),
            vmem((3 * latent, genes), BF16),
            vmem((8, slots), F32),
            vmem((1, slots), F32),
            vmem((m - 1, 1, slots), F32),
            vmem((genes, 2 * width + latent), F32),
            vmem((latent, slots), F32),
            vmem((genes, slots), BF16),
            vmem((genes, slots), BF16),
            vmem((genes, 3 * width), BF16),
            vmem((chips, 2, rows, wide), F32),
            vmem((chips, rows, wide), F32),
            vmem((chips - 1, rows, wide), F32),
            vmem((chips - 1, rows, wide), F32),
            vmem((128, wide), F32),
            vmem((wide, 128), F32),
            vmem((width, 128), F32),
            vmem((n, width, 128), F32),
            vmem((chips, 2, rows, 2 * latent), F32),
            vmem((chips, rows, 2 * latent), F32),
            vmem((chips - 1, rows, 2 * latent), F32),
            vmem((chips - 1, rows, 2 * latent), F32),
            vmem((latent, 128), F32),
            vmem((n, latent, 128), F32),
            vmem((m, 2 * latent, span), F32),
            vmem((m - 1, 2 * latent, span), F32),
            vmem((latent, span), F32),
            vmem((m, latent, span), F32),
            dma((n,)), dma((m - 1,)), dma((m - 1,)),
            dma((chips,)), dma((chips,)), dma((chips - 1,)), dma((chips - 1,)),
            dma((n - 1,)), dma((n - 1,)),
            dma((chips,)), dma((chips,)), dma((chips - 1,)), dma((chips - 1,)),
            dma((n - 1,)), dma((n - 1,)), dma((m - 1,)), dma((m - 1,)), dma((m - 1,)), dma((m - 1,)),
        ],
        compiler_params=params(collective_id=0, has_side_effects=True),
        name="step",
    )(
        counts, batch, live_cells.reshape(1, 1), knot, frac, cell_covariates, coefficients.T,
        batch_effect.T, factors.T, loadings.T,
    )
    beta, fs, ls = pl.pallas_call(
        pass_on, out_shape=shapes, in_specs=[VM] * 3, out_specs=(VM, VM, VM),
        compiler_params=params(), name="finish",
    )(*found)
    return beta.T, fs.T, ls.T


def local(n, m, *args):
    counts, cov, factors = args[0], args[5], args[8]
    genes, slots = counts.shape
    fits = (
        n == 8
        and m > 1
        and genes % (16 * n) == 0
        and genes // n <= 128
        and slots % (128 * m) == 0
        and cov.shape[0] == SPL
        and factors.shape[1] == 64
    )
    if fits:
        return local_fused(n, m, *args)
    return local_plain(*args)


def solution(mesh):
    placed = (
        P("gene", "cell"),
        P("cell"),
        P("cell"),
        P("cell"),
        P("cell"),
        P(None, "cell"),
        P("gene", None),
        P("gene", None),
        P("cell", None),
        P("gene", None),
    )
    return jax.shard_map(
        functools.partial(local, mesh.shape["cell"], mesh.shape["gene"]),
        mesh=mesh,
        in_specs=placed,
        out_specs=(P("gene", None), P("cell", None), P("gene", None)),
        check_vma=False,
    )
```

```python
import functools

import jax
import jax.numpy as jnp
from jax import lax
from jax.experimental import pallas as pl
from jax.experimental.pallas import tpu as pltpu
from jax.sharding import PartitionSpec as P

GENES = 3072
SPL = 16
BATCHES = 64


ridge_weight = 1.0


def design_rows(knot_bin, depth_frac, cell_covariates):
    levels = jnp.arange(SPL, dtype=jnp.int32)[:, None]
    fraction = depth_frac[None, :]
    hat_basis = jnp.where(levels == knot_bin[None, :], 1.0 - fraction, 0.0)
    hat_basis = hat_basis + jnp.where(levels == knot_bin[None, :] + 1, fraction, 0.0)
    return jnp.concatenate([hat_basis, cell_covariates], axis=0)


def newton_solve(gram_flat, score):
    columns = score.shape[-1]
    identity = jnp.eye(columns, dtype=gram_flat.dtype)
    system = gram_flat.reshape(-1, columns, columns) + ridge_weight * identity
    factor_lower = jnp.linalg.cholesky(system)
    middle = jax.scipy.linalg.solve_triangular(factor_lower, score[..., None], lower=True)
    return jax.scipy.linalg.solve_triangular(factor_lower, middle, lower=True, trans=1)[..., 0]


def local_plain(
    counts,
    batch_id,
    live_cells,
    knot_bin,
    depth_frac,
    cell_covariates,
    coefficients,
    batch_effect,
    factors,
    loadings,
):
    highest = lax.Precision.HIGHEST
    contract = (((1,), (1,)), ((), ()))
    observed = counts.astype(jnp.float32)
    totals = lax.psum(jnp.sum(observed, axis=0), "gene")
    offset = jnp.log((1.0 + totals) / GENES)
    slot_count = observed.shape[1]
    live_mask = (jnp.arange(slot_count, dtype=jnp.int32) < live_cells[0]).astype(jnp.float32)
    design = design_rows(knot_bin, depth_frac, cell_covariates)
    columns = design.shape[0]
    onehot = (jnp.arange(BATCHES, dtype=jnp.int32)[:, None] == batch_id[None, :]).astype(
        jnp.float32
    )
    stacked = jnp.concatenate([design, onehot], axis=0)
    linear = jnp.dot(
        jnp.concatenate([coefficients, batch_effect], axis=1), stacked, precision=highest
    )
    latent = lax.dot_general(loadings, factors, contract, preferred_element_type=jnp.float32)
    linear_pred = offset[None, :] + linear + latent
    expected = jnp.exp(linear_pred)
    weight = expected * live_mask
    residual = (observed - expected) * live_mask
    pairs = (design[:, None, :] * design[None, :, :]).reshape(columns * columns, slot_count)
    gram_part = lax.dot_general(weight, pairs, contract, precision=highest)
    score_part = lax.dot_general(residual, design, contract, precision=highest)
    gram_share, score_share = (
        lax.psum_scatter(gram_part, "cell", scatter_dimension=0, tiled=True),
        lax.psum_scatter(score_part, "cell", scatter_dimension=0, tiled=True),
    )
    step_share = newton_solve(gram_share, score_share)
    beta_step = lax.all_gather(step_share, "cell", axis=0, tiled=True)
    expected_next = jnp.exp(linear_pred + jnp.dot(beta_step, design, precision=highest))
    weight_next = expected_next * live_mask
    residual_next = (observed - expected_next) * live_mask
    factors_wide = factors.astype(jnp.float32)
    loads_wide = loadings.astype(jnp.float32)
    grad_load = jnp.dot(residual_next, factors_wide, precision=highest)
    curv_load = jnp.dot(weight_next, factors_wide * factors_wide, precision=highest)
    back = (((0,), (0,)), ((), ()))
    grad_fact = lax.dot_general(residual_next, loads_wide, back, precision=highest)
    curv_fact = lax.dot_general(weight_next, loads_wide * loads_wide, back, precision=highest)
    grad_load, curv_load = lax.psum((grad_load, curv_load), "cell")
    grad_fact, curv_fact = lax.psum((grad_fact, curv_fact), "gene")
    factor_step = grad_fact / (curv_fact + 1.0)
    loading_score = grad_load / jnp.sqrt(curv_load + 1.0)
    return (beta_step, factor_step, loading_score)


MESH = pl.DeviceIdType.MESH
F32, BF16 = jnp.float32, jnp.bfloat16
VM = pl.BlockSpec(memory_space=pltpu.VMEM)
ROWS_BY_ROWS = (((1,), (1,)), ((), ()))
ACROSS = (((1,), (0,)), ((), ()))
DOWN = (((0,), (0,)), ((), ()))
LIMIT = 40 * 1024 * 1024


def split(x):
    high = x.astype(BF16)
    return high, (x - high.astype(F32)).astype(BF16)


def mul(a, b, dims):
    return lax.dot_general(a, b, dims, preferred_element_type=F32)


def remote(src, dst, send, recv, where):
    return pltpu.make_async_remote_copy(
        src_ref=src, dst_ref=dst, send_sem=send, recv_sem=recv, device_id=where, device_id_type=MESH
    )


def meet_signal(groups):
    barrier = pltpu.get_barrier_semaphore()
    count = 0
    for axis, n in groups:
        me = lax.axis_index(axis)
        for d in range(1, n):
            pl.semaphore_signal(
                barrier, inc=1, device_id={axis: lax.rem(me + d, n)}, device_id_type=MESH
            )
        count += n - 1
    return lambda: pl.semaphore_wait(barrier, count)


def design_of(knot_ref, frac_ref, cov_ref):
    slots = knot_ref.shape[1]
    levels = lax.broadcasted_iota(jnp.int32, (SPL, slots), 0)
    knot, frac = knot_ref[...], frac_ref[...]
    hats = jnp.where(levels == knot, 1.0 - frac, 0.0)
    hats = hats + jnp.where(levels == knot + 1, frac, 0.0)
    return hats, cov_ref[...]


def build_pairs(hats, cov, pair_hi, pair_lo):
    slots = hats.shape[1]
    ncov = cov.shape[0]
    half = ncov // 2

    def put(at, block):
        high, low = split(block)
        pair_hi[at : at + block.shape[0]] = high
        pair_lo[at : at + block.shape[0]] = low

    at = 0
    for p in range(SPL):
        put(at, hats[p : p + 1] * cov)
        at += ncov
    for i in range(half):
        put(at, cov[i : i + 1] * cov)
        at += ncov
    for i in range(half, ncov, 2):
        put(
            at,
            jnp.concatenate(
                [cov[i : i + 1] * cov[half:], cov[i + 1 : i + 2] * cov[half:]], axis=0
            ),
        )
        at += ncov
    put(at, hats * hats)
    at += SPL
    later = jnp.concatenate([hats[1:], jnp.zeros((1, slots), F32)], axis=0)
    put(at, hats * later)
    at += SPL
    put(at, jnp.zeros((SPL + ncov, slots), F32))


def solve(g, x):
    half = SPL // 2
    cov_at, low_at, hat_at = SPL * SPL, SPL * SPL + half * SPL, SPL * SPL + half * SPL + half * half
    off_at, score_at = hat_at + SPL, hat_at + 2 * SPL
    spot = lax.broadcasted_iota(jnp.int32, (half, g.shape[1]), 0)

    def one(block, i):
        return block[i : i + 1]

    lo = {}
    hi = {}
    for i in range(SPL):
        unit = jnp.where(spot == i % half, ridge_weight, 0.0)
        if i < half:
            lo[i] = g[cov_at + i * SPL : cov_at + i * SPL + half] + unit
            hi[i] = g[cov_at + i * SPL + half : cov_at + (i + 1) * SPL]
        else:
            hi[i] = g[low_at + (i - half) * half : low_at + (i - half + 1) * half] + unit
    b_lo = g[score_at + SPL : score_at + SPL + half]
    b_hi = g[score_at + SPL + half : score_at + 2 * SPL]
    sums_lo, sums_hi = g[0:half], g[half:SPL]
    for p in range(1, SPL):
        sums_lo = sums_lo + g[p * SPL : p * SPL + half]
        sums_hi = sums_hi + g[p * SPL + half : (p + 1) * SPL]
    b_lo, b_hi = b_lo - sums_lo, b_hi - sums_hi
    pivot_inv, edge, side_lo, side_hi, rest = [], [], [], [], []
    for p in range(SPL):
        own = g[hat_at + p : hat_at + p + 1]
        after = g[off_at + p : off_at + p + 1]
        d = own + ridge_weight
        u_lo = g[p * SPL : p * SPL + half]
        u_hi = g[p * SPL + half : (p + 1) * SPL]
        b = g[score_at + p : score_at + p + 1] - own - after
        if p > 0:
            b = b - edge[-1]
            ratio = edge[-1] * pivot_inv[-1]
            d = d - ratio * edge[-1]
            u_lo = u_lo - ratio * side_lo[-1]
            u_hi = u_hi - ratio * side_hi[-1]
            b = b - ratio * rest[-1]
        inv = 1.0 / d
        pivot_inv.append(inv)
        edge.append(after)
        side_lo.append(u_lo)
        side_hi.append(u_hi)
        rest.append(b)
        scaled_lo, scaled_hi = u_lo * inv, u_hi * inv
        b_lo = b_lo - scaled_lo * b
        b_hi = b_hi - scaled_hi * b
        for i in range(SPL):
            if i < half:
                f = one(scaled_lo, i)
                lo[i] = lo[i] - f * u_lo
            else:
                f = one(scaled_hi, i - half)
            hi[i] = hi[i] - f * u_hi
    c_inv, c_rest = [], []
    for j in range(SPL):
        if j < half:
            inv = 1.0 / one(lo[j], j)
            b = one(b_lo, j)
            s_lo = lo[j] * inv
            b_lo = b_lo - s_lo * b
        else:
            inv = 1.0 / one(hi[j], j - half)
            b = one(b_hi, j - half)
        s_hi = hi[j] * inv
        b_hi = b_hi - s_hi * b
        c_inv.append(inv)
        c_rest.append(b)
        for i in range(j + 1, SPL):
            if i < half:
                f = one(s_lo, i)
                lo[i] = lo[i] - f * lo[j]
            else:
                f = one(s_hi, i - half)
            hi[i] = hi[i] - f * hi[j]
    for j in reversed(range(SPL)):
        found = c_rest[j] * c_inv[j]
        x[SPL + j : SPL + j + 1] = found
        for i in range(j):
            c_rest[i] = c_rest[i] - (one(hi[i], j - half) if j >= half else one(lo[i], j)) * found
    x_lo, x_hi = x[SPL : SPL + half], x[SPL + half : 2 * SPL]
    after = None
    for p in reversed(range(SPL)):
        gone = jnp.sum(side_lo[p] * x_lo + side_hi[p] * x_hi, axis=0, keepdims=True)
        b = rest[p] - gone
        if after is not None:
            b = b - edge[p] * after
        after = b * pivot_inv[p]
        x[p : p + 1] = after


def all_kernel(
    n, m, counts_hbm, batch_hbm, live_ref, knot_hbm, frac_hbm, cov_hbm, coef_hbm, shift_hbm,
    factors_hbm, loads_hbm, beta_ref, fs_ref, ls_ref,
    batch_ref, knot_ref, frac_ref, cov_ref, coef_ref, shift_ref, factors_ref, loads_ref,
    counts, lin, rhs, pair_hi, pair_lo, tally, f_all, l_all, extra, tot_out, tot_in, known_c, known_f,
    w_hi, w_lo, lhs_ref, g, g_pair, g_out, g_side, g_far, tall, turned, mine, theirs,
    gl, l_pair, l_out, l_far, my_l, their_l, gf, z_in, z_relay, z_sum, my_f, their_f,
    c_sem, i_sem, t_send, t_recv, gp_send, gp_recv, gs_send, gs_recv, gf_send, gf_recv,
    b_send, b_recv, lp_send, lp_recv, lf_send, lf_recv, ol_send, ol_recv, z_send, z_recv,
    of_send, of_recv,
):
    cell, gene = lax.axis_index("cell"), lax.axis_index("gene")
    core, chip = lax.rem(cell, 2), cell // 2
    chips = n // 2
    genes, slots = counts.shape
    block = genes // chips
    rows = genes // n
    latent = loads_ref.shape[0]
    span = slots // m
    arrive = meet_signal((("cell", n), ("gene", m)))
    loads_in = []
    for i in range(n):
        at = pl.ds(i * rows, rows)
        loads_in.append(pltpu.make_async_copy(counts_hbm.at[at], counts.at[at], c_sem.at[i]))
        loads_in[-1].start()
    small = []
    for i, (source, target) in enumerate(
        (
            (batch_hbm, batch_ref), (knot_hbm, knot_ref), (frac_hbm, frac_ref), (cov_hbm, cov_ref),
            (coef_hbm, coef_ref), (shift_hbm, shift_ref), (factors_hbm, factors_ref),
            (loads_hbm, loads_ref),
        )
    ):
        small.append(pltpu.make_async_copy(source, target, i_sem.at[i]))
        small[-1].start()
    part = None
    for i in range(n):
        loads_in[i].wait()
        piece = jnp.sum(counts[i * rows : (i + 1) * rows].reshape(rows // 8, 8, slots), axis=0)
        part = piece if part is None else part + piece
    tot_out[...] = jnp.sum(part, axis=0, keepdims=True).astype(F32)
    for copy in small:
        copy.wait()
    arrive()
    tot = []
    for d in range(1, m):
        tot.append(
            remote(
                tot_out, tot_in.at[d - 1], t_send.at[d - 1], t_recv.at[d - 1],
                {"gene": lax.rem(gene + d, m)},
            )
        )
        tot[-1].start()

    hats, cov = design_of(knot_ref, frac_ref, cov_ref)
    width = hats.shape[0] + cov.shape[0]
    design_hi, design_lo = split(jnp.concatenate([hats, cov], axis=0))
    hot = lax.broadcasted_iota(jnp.int32, (BATCHES, slots), 0) == batch_ref[...]
    hot = jnp.where(hot, 1.0, 0.0).astype(BF16)
    rhs[0:width] = design_hi
    rhs[width : 2 * width] = design_hi
    rhs[2 * width : 3 * width] = design_lo
    rhs[3 * width : 3 * width + BATCHES] = hot
    rhs[3 * width + BATCHES : 3 * width + 2 * BATCHES] = hot
    rhs[3 * width + 2 * BATCHES :] = factors_ref[...]
    coef_hi, coef_lo = split(coef_ref[...])
    shift_hi, shift_lo = split(shift_ref[...])
    lhs = jnp.concatenate([coef_hi, coef_lo, coef_hi, shift_hi, shift_lo, loads_ref[...]], axis=0)
    lin[...] = mul(lhs, rhs[...], DOWN)
    build_pairs(hats, cov, pair_hi, pair_lo)
    live = lax.broadcasted_iota(jnp.int32, (1, slots), 1) < live_ref[0]
    mask = jnp.where(live, 1.0, 0.0)
    mask_bf = mask.astype(BF16)
    factors_live = factors_ref[...].astype(F32) * mask
    tally[0:width] = design_hi * mask_bf
    tally[width : 2 * width] = design_lo * mask_bf
    tally[2 * width :] = factors_live.astype(BF16)
    known_c[...] = mul(counts[...].astype(F32).astype(BF16), tally[...], ROWS_BY_ROWS)

    total = tot_out[...]
    for d in range(1, m):
        tot[d - 1].wait()
        total = total + tot_in[d - 1]
    extra[0:1] = jnp.where(live, jnp.log((1.0 + total) / GENES), -1e30)

    beside, above = chip + 1 - 2 * lax.rem(chip, 2), lax.rem(chip + 2, chips)
    places = [chips - 1 - chip, beside, above, chip]
    partner = cell + 1 - 2 * core
    wide = g.shape[3]
    cut = rows // 2
    upper, lower = slice(0, cut), slice(cut, rows)

    def gram_chunk(j):
        at = pl.ds(pl.multiple_of(places[j] * block, block), block)
        linear = lin[at] + extra[0:1]
        lin[at] = linear
        high, low = split(jnp.exp(linear))
        both = mul(jnp.concatenate([high, low], axis=0), pair_hi[...], ROWS_BY_ROWS)
        gram = both[:block] + both[block:] + mul(high, pair_lo[...], ROWS_BY_ROWS)
        counted = known_c[at, 0:width] + known_c[at, width : 2 * width]
        g[j, :, :, : wide - width] = gram[:, : wide - width].reshape(2, rows, wide - width)
        g[j, :, :, wide - width :] = counted.reshape(2, rows, width)
        copy = remote(
            g.at[j, 1 - core], g_pair.at[j], gp_send.at[j], gp_recv.at[j], {"cell": partner}
        )
        copy.start()
        return copy

    def onward(j, part, target, send, recv, place):
        copy = remote(g_out.at[j, part], target, send, recv, {"cell": 2 * place + core})
        copy.start()
        return copy

    pair = [gram_chunk(0), gram_chunk(1)]
    pair[0].wait()
    g_out[0] = g[0, core] + g_pair[0]
    side = [
        onward(0, upper, g_side.at[0], gs_send.at[0], gs_recv.at[0], beside),
        onward(0, lower, g_side.at[1], gs_send.at[1], gs_recv.at[1], above),
    ]
    pair.append(gram_chunk(2))
    pair[1].wait()
    g_out[1, upper] = g[1, core, upper] + g_pair[1, upper]
    far = [onward(1, upper, g_far.at[0, upper], gf_send.at[0], gf_recv.at[0], beside)]
    pair.append(gram_chunk(3))
    pair[2].wait()
    g_out[2, lower] = g[2, core, lower] + g_pair[2, lower]
    far.append(onward(2, lower, g_far.at[1, lower], gf_send.at[1], gf_recv.at[1], above))

    f_hi, f_lo = split(factors_live * factors_live)
    f_all[0:latent] = tally[2 * width :]
    f_all[latent : 2 * latent] = f_hi
    f_all[2 * latent :] = f_lo
    loads_wide = loads_ref[...].astype(F32)
    l_hi, l_lo = split(loads_wide * loads_wide)
    l_all[0:latent] = loads_ref[...]
    l_all[latent : 2 * latent] = l_hi
    l_all[2 * latent :] = l_lo

    side[1].wait()
    g_out[1, lower] = g[1, core, lower] + g_pair[1, lower] + g_side[1]
    far.append(onward(1, lower, g_far.at[0, lower], gf_send.at[2], gf_recv.at[2], beside))
    side[0].wait()
    g_out[2, upper] = g[2, core, upper] + g_pair[2, upper] + g_side[0]
    far.append(onward(2, upper, g_far.at[1, upper], gf_send.at[3], gf_recv.at[3], above))
    known_f[...] = mul(l_all[0:latent], counts[...].astype(F32).astype(BF16), ACROSS) * mask
    pair[3].wait()
    total = g[3, core] + g_pair[3]
    for copy in far:
        copy.wait()
    total = total + g_far[0] + g_far[1]
    tall[0:rows] = total
    if rows < 128:
        tall[rows:128] = jnp.zeros((128 - rows, wide), F32)
    turned[...] = tall[...].T
    solve(turned, mine)
    out = []
    for d in range(1, n):
        out.append(
            remote(
                mine, theirs.at[cell], b_send.at[d - 1], b_recv.at[d - 1],
                {"cell": lax.rem(cell + d, n)},
            )
        )
        out[-1].start()
    theirs[cell] = mine[...]
    for d in range(1, n):
        out[d - 1].wait()
    for o in range(n):
        beta_ref[:, o * rows : (o + 1) * rows] = theirs[o, :, :rows]
    beta_hi, beta_lo = split(beta_ref[...])
    lhs_ref[...] = jnp.concatenate([beta_hi, beta_lo, beta_hi], axis=0).astype(F32).T.astype(BF16)

    row = gene // 2
    middle = lax.rem(gene + row, 2)
    near = gene + 1 - 2 * lax.rem(gene, 2)
    far_mid, far_end = 2 - row, 3 - 3 * row

    def fact_chunk(j, owner):
        cols = pl.ds(pl.multiple_of(owner * span, span), span)
        delta = mul(lhs_ref[...], rhs[0 : 3 * width, cols], ACROSS)
        high, low = split(jnp.exp(lin[:, cols] + delta))
        w_hi[:, cols] = high
        w_lo[:, cols] = low
        first = mul(l_all[...], high, ACROSS)
        second = mul(l_all[0 : 2 * latent], low, ACROSS)
        gf[j, :latent] = known_f[:, cols] - first[:latent] - second[:latent]
        gf[j, latent:] = first[latent : 2 * latent] + first[2 * latent :] + second[latent:]

    def along(j, target, k, slot, place):
        return remote(gf.at[j], target, z_send.at[k], z_recv.at[slot], {"gene": place})

    relay = along(0, z_relay, 0, 3, near)
    joined = along(0, z_in.at[1], 0, 1, far_mid)
    straight = along(1, z_in.at[2 - middle], 1, 2 - middle, far_end)
    close = along(2, z_in.at[0], 2, 0, near)
    fact_chunk(0, far_mid)

    @pl.when(middle == 0)
    def _():
        relay.start()

    fact_chunk(1, far_end)
    straight.start()
    fact_chunk(2, near)
    close.start()
    fact_chunk(3, gene)

    lpair, lfar = [], []

    def hand_on(j):
        lpair[j].wait()
        l_out[j] = gl[j, core] + l_pair[j]
        lfar.append(
            remote(
                l_out.at[j], l_far.at[j], lf_send.at[j], lf_recv.at[j],
                {"cell": 2 * places[j] + core},
            )
        )
        lfar[-1].start()

    for j in range(chips):
        at = pl.ds(pl.multiple_of(places[j] * block, block), block)
        first = mul(w_hi[at], f_all[...], ROWS_BY_ROWS)
        second = mul(w_lo[at], f_all[0 : 2 * latent], ROWS_BY_ROWS)
        grad = known_c[at, 2 * width :] - first[:, :latent] - second[:, :latent]
        curv = first[:, latent : 2 * latent] + first[:, 2 * latent :] + second[:, latent:]
        gl[j] = jnp.concatenate([grad, curv], axis=1).reshape(2, rows, 2 * latent)
        lpair.append(
            remote(gl.at[j, 1 - core], l_pair.at[j], lp_send.at[j], lp_recv.at[j], {"cell": partner})
        )
        lpair[-1].start()
        if j > 0:
            hand_on(j - 1)

    @pl.when(middle == 1)
    def _():
        relay.wait_recv()
        gf[0] = gf[0] + z_relay[...]
        joined.start()

    lpair[-1].wait()
    total = gl[chips - 1, core] + l_pair[chips - 1]
    for j in range(chips - 1):
        lfar[j].wait()
        total = total + l_far[j]
    if rows < 128:
        total = jnp.concatenate([total, jnp.zeros((128 - rows, 2 * latent), F32)], axis=0)
    total = total.T
    my_l[...] = total[:latent] / jnp.sqrt(total[latent:] + 1.0)
    out_l = []
    for d in range(1, n):
        out_l.append(
            remote(
                my_l, their_l.at[cell], ol_send.at[d - 1], ol_recv.at[d - 1],
                {"cell": lax.rem(cell + d, n)},
            )
        )
        out_l[-1].start()
    their_l[cell] = my_l[...]

    close.wait()
    z_sum[...] = gf[3] + z_in[0]

    @pl.when(middle == 0)
    def _():
        straight.wait()
        z_sum[...] += z_in[2]
        joined.wait_recv()
        relay.wait_send()

    @pl.when(middle == 1)
    def _():
        straight.wait_send()
        joined.wait()

    total = z_sum[...] + z_in[1]
    my_f[...] = total[:latent] / (total[latent:] + 1.0)

    def give(source, owner, k, place):
        return remote(source, their_f.at[owner], of_send.at[k], of_recv.at[owner], {"gene": place})

    give_a = give(my_f, gene, 0, far_end + middle * (far_mid - far_end))
    give_b = give(my_f, gene, 1, far_mid + middle * (near - far_mid))
    give_c = give(my_f, gene, 2, near)
    pass_c = give(their_f.at[far_mid], far_mid, 2, near)
    give_a.start()
    give_b.start()

    @pl.when(middle == 0)
    def _():
        give_c.start()

    their_f[gene] = my_f[...]

    @pl.when(middle == 1)
    def _():
        pass_c.wait_recv()
        pass_c.start()

    for d in range(1, n):
        out_l[d - 1].wait()
    for o in range(n):
        ls_ref[:, o * rows : (o + 1) * rows] = their_l[o, :, :rows]

    give(my_f, near, 0, near).wait_recv()
    give(my_f, far_end, 0, near).wait_recv()

    @pl.when(middle == 0)
    def _():
        pass_c.wait_recv()

    give_a.wait_send()
    give_b.wait_send()
    give_c.wait_send()
    for o in range(m):
        fs_ref[:, o * span : (o + 1) * span] = their_f[o]


def pass_on(*refs):
    count = len(refs) // 2
    for source, target in zip(refs[:count], refs[count:]):
        target[...] = source[...]


def local_fused(
    n, m, counts, batch_id, live_cells, knot_bin, depth_frac, cell_covariates, coefficients,
    batch_effect, factors, loadings,
):
    genes, slots = counts.shape
    rows, span, latent = genes // n, slots // m, factors.shape[1]
    ncov = cell_covariates.shape[0]
    width = SPL + ncov
    wide = SPL * ncov + ncov * ncov * 3 // 4 + 2 * SPL + width
    chips = n // 2
    dma = pltpu.SemaphoreType.DMA
    shape = jax.ShapeDtypeStruct
    vmem = pltpu.VMEM

    def params(**kw):
        return pltpu.CompilerParams(vmem_limit_bytes=LIMIT, **kw)

    def stay(x):
        return pltpu.with_memory_space_constraint(x, pltpu.HBM)

    knot, frac, batch = (v.reshape(1, slots) for v in (knot_bin, depth_frac, batch_id))
    shapes = (shape((width, genes), F32), shape((latent, slots), F32), shape((latent, genes), F32))
    there = pl.BlockSpec(memory_space=pl.ANY)
    found = pl.pallas_call(
        functools.partial(all_kernel, n, m),
        out_shape=shapes,
        in_specs=[there, there, pl.BlockSpec(memory_space=pltpu.SMEM)] + [there] * 7,
        out_specs=(VM, VM, VM),
        scratch_shapes=[
            vmem((1, slots), jnp.int32),
            vmem((1, slots), jnp.int32),
            vmem((1, slots), F32),
            vmem((ncov, slots), F32),
            vmem((width, genes), F32),
            vmem((BATCHES, genes), F32),
            vmem((latent, slots), BF16),
            vmem((latent, genes), BF16),
            vmem((genes, slots), jnp.int32),
            vmem((genes, slots), F32),
            vmem((3 * width + 2 * BATCHES + latent, slots), BF16),
            vmem((wide, slots), BF16),
            vmem((wide, slots), BF16),
            vmem((2 * width + latent, slots), BF16),
            vmem((3 * latent, slots), BF16),
            vmem((3 * latent, genes), BF16),
            vmem((8, slots), F32),
            vmem((1, slots), F32),
            vmem((m - 1, 1, slots), F32),
            vmem((genes, 2 * width + latent), F32),
            vmem((latent, slots), F32),
            vmem((genes, slots), BF16),
            vmem((genes, slots), BF16),
            vmem((genes, 3 * width), BF16),
            vmem((chips, 2, rows, wide), F32),
            vmem((chips, rows, wide), F32),
            vmem((chips - 1, rows, wide), F32),
            vmem((2, rows // 2, wide), F32),
            vmem((2, rows, wide), F32),
            vmem((128, wide), F32),
            vmem((wide, 128), F32),
            vmem((width, 128), F32),
            vmem((n, width, 128), F32),
            vmem((chips, 2, rows, 2 * latent), F32),
            vmem((chips, rows, 2 * latent), F32),
            vmem((chips - 1, rows, 2 * latent), F32),
            vmem((chips - 1, rows, 2 * latent), F32),
            vmem((latent, 128), F32),
            vmem((n, latent, 128), F32),
            vmem((m, 2 * latent, span), F32),
            vmem((m - 1, 2 * latent, span), F32),
            vmem((2 * latent, span), F32),
            vmem((2 * latent, span), F32),
            vmem((latent, span), F32),
            vmem((m, latent, span), F32),
            dma((n,)), dma((8,)), dma((m - 1,)), dma((m - 1,)),
            dma((chips,)), dma((chips,)), dma((2,)), dma((2,)), dma((4,)), dma((4,)),
            dma((n - 1,)), dma((n - 1,)),
            dma((chips,)), dma((chips,)), dma((chips - 1,)), dma((chips - 1,)),
            dma((n - 1,)), dma((n - 1,)), dma((m - 1,)), dma((m,)), dma((m - 1,)), dma((m,)),
        ],
        compiler_params=params(collective_id=0, has_side_effects=True),
        name="step",
    )(
        stay(counts), stay(batch), live_cells, stay(knot), stay(frac), stay(cell_covariates),
        stay(coefficients.T), stay(batch_effect.T), stay(factors.T), stay(loadings.T),
    )
    beta, fs, ls = pl.pallas_call(
        pass_on, out_shape=shapes, in_specs=[VM] * 3, out_specs=(VM, VM, VM),
        compiler_params=params(), name="finish",
    )(*found)
    return beta.T, fs.T, ls.T


def local(n, m, *args):
    counts, cov, factors = args[0], args[5], args[8]
    genes, slots = counts.shape
    fits = (
        n == 8
        and m == 4
        and genes % (16 * n) == 0
        and genes // n <= 128
        and slots % (128 * m) == 0
        and cov.shape[0] == SPL
        and factors.shape[1] == 64
    )
    if fits:
        return local_fused(n, m, *args)
    return local_plain(*args)


def solution(mesh):
    placed = (
        P("gene", "cell"),
        P("cell"),
        P("cell"),
        P("cell"),
        P("cell"),
        P(None, "cell"),
        P("gene", None),
        P("gene", None),
        P("cell", None),
        P("gene", None),
    )
    return jax.shard_map(
        functools.partial(local, mesh.shape["cell"], mesh.shape["gene"]),
        mesh=mesh,
        in_specs=placed,
        out_specs=(P("gene", None), P("cell", None), P("gene", None)),
        check_vma=False,
    )
```

```python
import functools

import jax
import jax.numpy as jnp
from jax import lax
from jax.experimental import pallas as pl
from jax.experimental.pallas import tpu as pltpu
from jax.sharding import PartitionSpec as P

GENES = 3072
SPL = 16
BATCHES = 64


ridge_weight = 1.0


def design_rows(knot_bin, depth_frac, cell_covariates):
    levels = jnp.arange(SPL, dtype=jnp.int32)[:, None]
    fraction = depth_frac[None, :]
    hat_basis = jnp.where(levels == knot_bin[None, :], 1.0 - fraction, 0.0)
    hat_basis = hat_basis + jnp.where(levels == knot_bin[None, :] + 1, fraction, 0.0)
    return jnp.concatenate([hat_basis, cell_covariates], axis=0)


def newton_solve(gram_flat, score):
    columns = score.shape[-1]
    identity = jnp.eye(columns, dtype=gram_flat.dtype)
    system = gram_flat.reshape(-1, columns, columns) + ridge_weight * identity
    factor_lower = jnp.linalg.cholesky(system)
    middle = jax.scipy.linalg.solve_triangular(factor_lower, score[..., None], lower=True)
    return jax.scipy.linalg.solve_triangular(factor_lower, middle, lower=True, trans=1)[..., 0]


def local_plain(
    counts,
    batch_id,
    live_cells,
    knot_bin,
    depth_frac,
    cell_covariates,
    coefficients,
    batch_effect,
    factors,
    loadings,
):
    highest = lax.Precision.HIGHEST
    contract = (((1,), (1,)), ((), ()))
    observed = counts.astype(jnp.float32)
    totals = lax.psum(jnp.sum(observed, axis=0), "gene")
    offset = jnp.log((1.0 + totals) / GENES)
    slot_count = observed.shape[1]
    live_mask = (jnp.arange(slot_count, dtype=jnp.int32) < live_cells[0]).astype(jnp.float32)
    design = design_rows(knot_bin, depth_frac, cell_covariates)
    columns = design.shape[0]
    onehot = (jnp.arange(BATCHES, dtype=jnp.int32)[:, None] == batch_id[None, :]).astype(
        jnp.float32
    )
    stacked = jnp.concatenate([design, onehot], axis=0)
    linear = jnp.dot(
        jnp.concatenate([coefficients, batch_effect], axis=1), stacked, precision=highest
    )
    latent = lax.dot_general(loadings, factors, contract, preferred_element_type=jnp.float32)
    linear_pred = offset[None, :] + linear + latent
    expected = jnp.exp(linear_pred)
    weight = expected * live_mask
    residual = (observed - expected) * live_mask
    pairs = (design[:, None, :] * design[None, :, :]).reshape(columns * columns, slot_count)
    gram_part = lax.dot_general(weight, pairs, contract, precision=highest)
    score_part = lax.dot_general(residual, design, contract, precision=highest)
    gram_share, score_share = (
        lax.psum_scatter(gram_part, "cell", scatter_dimension=0, tiled=True),
        lax.psum_scatter(score_part, "cell", scatter_dimension=0, tiled=True),
    )
    step_share = newton_solve(gram_share, score_share)
    beta_step = lax.all_gather(step_share, "cell", axis=0, tiled=True)
    expected_next = jnp.exp(linear_pred + jnp.dot(beta_step, design, precision=highest))
    weight_next = expected_next * live_mask
    residual_next = (observed - expected_next) * live_mask
    factors_wide = factors.astype(jnp.float32)
    loads_wide = loadings.astype(jnp.float32)
    grad_load = jnp.dot(residual_next, factors_wide, precision=highest)
    curv_load = jnp.dot(weight_next, factors_wide * factors_wide, precision=highest)
    back = (((0,), (0,)), ((), ()))
    grad_fact = lax.dot_general(residual_next, loads_wide, back, precision=highest)
    curv_fact = lax.dot_general(weight_next, loads_wide * loads_wide, back, precision=highest)
    grad_load, curv_load = lax.psum((grad_load, curv_load), "cell")
    grad_fact, curv_fact = lax.psum((grad_fact, curv_fact), "gene")
    factor_step = grad_fact / (curv_fact + 1.0)
    loading_score = grad_load / jnp.sqrt(curv_load + 1.0)
    return (beta_step, factor_step, loading_score)


MESH = pl.DeviceIdType.MESH
F32, BF16 = jnp.float32, jnp.bfloat16
VM = pl.BlockSpec(memory_space=pltpu.VMEM)
ROWS_BY_ROWS = (((1,), (1,)), ((), ()))
ACROSS = (((1,), (0,)), ((), ()))
DOWN = (((0,), (0,)), ((), ()))
LIMIT = 40 * 1024 * 1024


def split(x):
    high = x.astype(BF16)
    return high, (x - high.astype(F32)).astype(BF16)


def mul(a, b, dims):
    return lax.dot_general(a, b, dims, preferred_element_type=F32)


def remote(src, dst, send, recv, where):
    return pltpu.make_async_remote_copy(
        src_ref=src, dst_ref=dst, send_sem=send, recv_sem=recv, device_id=where, device_id_type=MESH
    )


def meet_signal(groups):
    barrier = pltpu.get_barrier_semaphore()
    count = 0
    for axis, n in groups:
        me = lax.axis_index(axis)
        for d in range(1, n):
            pl.semaphore_signal(
                barrier, inc=1, device_id={axis: lax.rem(me + d, n)}, device_id_type=MESH
            )
        count += n - 1
    return lambda: pl.semaphore_wait(barrier, count)


def design_of(knot_ref, frac_ref, cov_ref):
    slots = knot_ref.shape[1]
    levels = lax.broadcasted_iota(jnp.int32, (SPL, slots), 0)
    knot, frac = knot_ref[...], frac_ref[...]
    hats = jnp.where(levels == knot, 1.0 - frac, 0.0)
    hats = hats + jnp.where(levels == knot + 1, frac, 0.0)
    return hats, cov_ref[...]


def build_pairs(hats, cov, pair_hi, pair_lo):
    slots = hats.shape[1]
    ncov = cov.shape[0]
    half = ncov // 2

    def put(at, block):
        high, low = split(block)
        pair_hi[at : at + block.shape[0]] = high
        pair_lo[at : at + block.shape[0]] = low

    at = 0
    for p in range(SPL):
        put(at, hats[p : p + 1] * cov)
        at += ncov
    for i in range(half):
        put(at, cov[i : i + 1] * cov)
        at += ncov
    for i in range(half, ncov, 2):
        put(
            at,
            jnp.concatenate(
                [cov[i : i + 1] * cov[half:], cov[i + 1 : i + 2] * cov[half:]], axis=0
            ),
        )
        at += ncov
    put(at, hats * hats)
    at += SPL
    later = jnp.concatenate([hats[1:], jnp.zeros((1, slots), F32)], axis=0)
    put(at, hats * later)
    at += SPL
    put(at, jnp.zeros((SPL + ncov, slots), F32))


def solve(g, x):
    half = SPL // 2
    cov_at, low_at, hat_at = SPL * SPL, SPL * SPL + half * SPL, SPL * SPL + half * SPL + half * half
    off_at, score_at = hat_at + SPL, hat_at + 2 * SPL
    spot = lax.broadcasted_iota(jnp.int32, (half, g.shape[1]), 0)

    def one(block, i):
        return block[i : i + 1]

    lo = {}
    hi = {}
    for i in range(SPL):
        unit = jnp.where(spot == i % half, ridge_weight, 0.0)
        if i < half:
            lo[i] = g[cov_at + i * SPL : cov_at + i * SPL + half] + unit
            hi[i] = g[cov_at + i * SPL + half : cov_at + (i + 1) * SPL]
        else:
            hi[i] = g[low_at + (i - half) * half : low_at + (i - half + 1) * half] + unit
    b_lo = g[score_at + SPL : score_at + SPL + half]
    b_hi = g[score_at + SPL + half : score_at + 2 * SPL]
    sums_lo, sums_hi = g[0:half], g[half:SPL]
    for p in range(1, SPL):
        sums_lo = sums_lo + g[p * SPL : p * SPL + half]
        sums_hi = sums_hi + g[p * SPL + half : (p + 1) * SPL]
    b_lo, b_hi = b_lo - sums_lo, b_hi - sums_hi
    pivot_inv, edge, side_lo, side_hi, rest = [], [], [], [], []
    for p in range(SPL):
        own = g[hat_at + p : hat_at + p + 1]
        after = g[off_at + p : off_at + p + 1]
        d = own + ridge_weight
        u_lo = g[p * SPL : p * SPL + half]
        u_hi = g[p * SPL + half : (p + 1) * SPL]
        b = g[score_at + p : score_at + p + 1] - own - after
        if p > 0:
            b = b - edge[-1]
            ratio = edge[-1] * pivot_inv[-1]
            d = d - ratio * edge[-1]
            u_lo = u_lo - ratio * side_lo[-1]
            u_hi = u_hi - ratio * side_hi[-1]
            b = b - ratio * rest[-1]
        inv = 1.0 / d
        pivot_inv.append(inv)
        edge.append(after)
        side_lo.append(u_lo)
        side_hi.append(u_hi)
        rest.append(b)
        scaled_lo, scaled_hi = u_lo * inv, u_hi * inv
        b_lo = b_lo - scaled_lo * b
        b_hi = b_hi - scaled_hi * b
        for i in range(SPL):
            if i < half:
                f = one(scaled_lo, i)
                lo[i] = lo[i] - f * u_lo
            else:
                f = one(scaled_hi, i - half)
            hi[i] = hi[i] - f * u_hi
    c_inv, c_rest = [], []
    for j in range(SPL):
        if j < half:
            inv = 1.0 / one(lo[j], j)
            b = one(b_lo, j)
            s_lo = lo[j] * inv
            b_lo = b_lo - s_lo * b
        else:
            inv = 1.0 / one(hi[j], j - half)
            b = one(b_hi, j - half)
        s_hi = hi[j] * inv
        b_hi = b_hi - s_hi * b
        c_inv.append(inv)
        c_rest.append(b)
        for i in range(j + 1, SPL):
            if i < half:
                f = one(s_lo, i)
                lo[i] = lo[i] - f * lo[j]
            else:
                f = one(s_hi, i - half)
            hi[i] = hi[i] - f * hi[j]
    for j in reversed(range(SPL)):
        found = c_rest[j] * c_inv[j]
        x[SPL + j : SPL + j + 1] = found
        for i in range(j):
            c_rest[i] = c_rest[i] - (one(hi[i], j - half) if j >= half else one(lo[i], j)) * found
    x_lo, x_hi = x[SPL : SPL + half], x[SPL + half : 2 * SPL]
    after = None
    for p in reversed(range(SPL)):
        gone = jnp.sum(side_lo[p] * x_lo + side_hi[p] * x_hi, axis=0, keepdims=True)
        b = rest[p] - gone
        if after is not None:
            b = b - edge[p] * after
        after = b * pivot_inv[p]
        x[p : p + 1] = after


def all_kernel(
    n, m, counts_hbm, batch_hbm, live_ref, knot_hbm, frac_hbm, cov_hbm, coef_hbm, shift_hbm,
    factors_hbm, loads_hbm, beta_ref, fs_ref, ls_ref,
    batch_ref, knot_ref, frac_ref, cov_ref, factors_ref, loads_ref, p_own, p_all,
    counts, lin, rhs, pair_hi, pair_lo, tally, f_all, l_all, extra, tot_out, tot_in, known_c, known_f,
    cl_in, cl_own, cl_all, w_hi, w_lo, lhs_ref, g, g_pair, g_out, g_side, g_far, tall, turned, mine,
    b_all, b_cat, gl, l_pair, l_out, l_far, my_l, their_l, gf,
    c_sem, i_sem, t_send, t_recv, pz_send, pz_recv, px_send, px_recv, pp_send, pp_recv,
    gp_send, gp_recv, gs_send, gs_recv, gf_send, gf_recv, ci_send, ci_recv, ca_send, ca_recv,
    b_send, b_recv, bz_send, bz_recv, bx_send, bx_recv, bp_send, bp_recv,
    lp_send, lp_recv, lf_send, lf_recv, ol_send, ol_recv,
):
    cell, gene = lax.axis_index("cell"), lax.axis_index("gene")
    core, chip = lax.rem(cell, 2), cell // 2
    chips = n // 2
    genes, slots = counts.shape
    block = genes // chips
    rows = genes // n
    latent = loads_ref.shape[0]
    span = slots // m
    width = SPL + cov_hbm.shape[0]
    tall_p = p_own.shape[0]
    coef_ref, shift_ref = p_own.at[0:width], p_own.at[width : width + BATCHES]
    arrive = meet_signal((("cell", n), ("gene", m)))
    loads_in = []
    for i in range(n):
        at = pl.ds(i * rows, rows)
        loads_in.append(pltpu.make_async_copy(counts_hbm.at[at], counts.at[at], c_sem.at[i]))
        loads_in[-1].start()
    small = []
    for i, (source, target) in enumerate(
        (
            (batch_hbm, batch_ref), (knot_hbm, knot_ref), (frac_hbm, frac_ref), (cov_hbm, cov_ref),
            (coef_hbm, coef_ref), (shift_hbm, shift_ref), (factors_hbm, factors_ref),
            (loads_hbm, loads_ref),
        )
    ):
        small.append(pltpu.make_async_copy(source, target, i_sem.at[i]))
        small[-1].start()
    part = None
    for i in range(n):
        loads_in[i].wait()
        piece = jnp.sum(counts[i * rows : (i + 1) * rows].reshape(rows // 8, 8, slots), axis=0)
        part = piece if part is None else part + piece
    tot_out[...] = jnp.sum(part, axis=0, keepdims=True).astype(F32)
    for copy in small:
        copy.wait()
    p_own[width + BATCHES :] = loads_ref[...].astype(F32)
    arrive()
    tot = []
    for d in range(1, m):
        tot.append(
            remote(
                tot_out, tot_in.at[d - 1], t_send.at[d - 1], t_recv.at[d - 1],
                {"gene": lax.rem(gene + d, m)},
            )
        )
        tot[-1].start()

    line = gene // 2
    near = gene + 1 - 2 * lax.rem(gene, 2)
    others = [near, 2 - line, 3 - 3 * line]
    beside, above = chip + 1 - 2 * lax.rem(chip, 2), lax.rem(chip + 2, chips)
    places = [chips - 1 - chip, beside, above, chip]
    partner = cell + 1 - 2 * core
    deep, broad = tall_p // chips, genes // 2
    p_rows = pl.ds(pl.multiple_of(chip * deep, deep), deep)
    p_cols = pl.ds(pl.multiple_of(core * broad, broad), broad)
    p_line = []
    for i, z in enumerate(others):
        p_line.append(
            remote(
                p_own.at[p_rows, p_cols], p_all.at[gene, p_rows, p_cols], pz_send.at[i],
                pz_recv.at[gene], {"gene": z},
            )
        )
        p_line[-1].start()

    def p_landing(z):
        piece = p_all.at[z, p_rows, p_cols]
        return remote(piece, piece, pz_send.at[0], pz_recv.at[z], {"gene": near})

    p_plane = {}

    def p_forward(i):
        z = others[i]
        p_landing(z).wait_recv()
        for k in range(chips - 1):
            piece = p_all.at[z, p_rows, p_cols]
            p_plane[i, k] = remote(
                piece, piece, px_send.at[i, k], px_recv.at[i, k], {"cell": 2 * places[k] + core}
            )
            p_plane[i, k].start()

    hats, cov = design_of(knot_ref, frac_ref, cov_ref)
    design_hi, design_lo = split(jnp.concatenate([hats, cov], axis=0))
    hot = lax.broadcasted_iota(jnp.int32, (BATCHES, slots), 0) == batch_ref[...]
    hot = jnp.where(hot, 1.0, 0.0).astype(BF16)
    rhs[0:width] = design_hi
    rhs[width : 2 * width] = design_hi
    rhs[2 * width : 3 * width] = design_lo
    rhs[3 * width : 3 * width + BATCHES] = hot
    rhs[3 * width + BATCHES : 3 * width + 2 * BATCHES] = hot
    rhs[3 * width + 2 * BATCHES :] = factors_ref[...]
    coef_hi, coef_lo = split(coef_ref[...])
    shift_hi, shift_lo = split(shift_ref[...])
    lhs = jnp.concatenate([coef_hi, coef_lo, coef_hi, shift_hi, shift_lo, loads_ref[...]], axis=0)
    lin[...] = mul(lhs, rhs[...], DOWN)
    build_pairs(hats, cov, pair_hi, pair_lo)
    live = lax.broadcasted_iota(jnp.int32, (1, slots), 1) < live_ref[0]
    mask = jnp.where(live, 1.0, 0.0)
    mask_bf = mask.astype(BF16)
    factors_live = factors_ref[...].astype(F32) * mask
    tally[0:width] = design_hi * mask_bf
    tally[width : 2 * width] = design_lo * mask_bf
    tally[2 * width :] = factors_live.astype(BF16)
    known_c[...] = mul(counts[...].astype(F32).astype(BF16), tally[...], ROWS_BY_ROWS)

    total = tot_out[...]
    for d in range(1, m):
        tot[d - 1].wait()
        total = total + tot_in[d - 1]
    extra[0:1] = jnp.where(live, jnp.log((1.0 + total) / GENES), -1e30)

    wide = g.shape[3]
    cut = rows // 2
    upper, lower = slice(0, cut), slice(cut, rows)

    def gram_chunk(j):
        at = pl.ds(pl.multiple_of(places[j] * block, block), block)
        linear = lin[at] + extra[0:1]
        lin[at] = linear
        high, low = split(jnp.exp(linear))
        both = mul(jnp.concatenate([high, low], axis=0), pair_hi[...], ROWS_BY_ROWS)
        gram = both[:block] + both[block:] + mul(high, pair_lo[...], ROWS_BY_ROWS)
        counted = known_c[at, 0:width] + known_c[at, width : 2 * width]
        g[j, :, :, : wide - width] = gram[:, : wide - width].reshape(2, rows, wide - width)
        g[j, :, :, wide - width :] = counted.reshape(2, rows, width)
        copy = remote(
            g.at[j, 1 - core], g_pair.at[j], gp_send.at[j], gp_recv.at[j], {"cell": partner}
        )
        copy.start()
        return copy

    def onward(j, part, target, send, recv, place):
        copy = remote(g_out.at[j, part], target, send, recv, {"cell": 2 * place + core})
        copy.start()
        return copy

    p_forward(0)
    pair = [gram_chunk(0), gram_chunk(1)]
    pair[0].wait()
    g_out[0] = g[0, core] + g_pair[0]
    side = [
        onward(0, upper, g_side.at[0], gs_send.at[0], gs_recv.at[0], beside),
        onward(0, lower, g_side.at[1], gs_send.at[1], gs_recv.at[1], above),
    ]
    pair.append(gram_chunk(2))
    pair[1].wait()
    g_out[1, upper] = g[1, core, upper] + g_pair[1, upper]
    far = [onward(1, upper, g_far.at[0, upper], gf_send.at[0], gf_recv.at[0], beside)]
    pair.append(gram_chunk(3))
    pair[2].wait()
    g_out[2, lower] = g[2, core, lower] + g_pair[2, lower]
    far.append(onward(2, lower, g_far.at[1, lower], gf_send.at[1], gf_recv.at[1], above))

    f_hi, f_lo = split(factors_live * factors_live)
    f_all[0:latent] = tally[2 * width :]
    f_all[latent : 2 * latent] = f_hi
    f_all[2 * latent :] = f_lo
    loads_wide = loads_ref[...].astype(F32)
    l_hi, l_lo = split(loads_wide * loads_wide)
    l_all[0:latent] = loads_ref[...]
    l_all[latent : 2 * latent] = l_hi
    l_all[2 * latent :] = l_lo

    known_f[...] = mul(l_all[0:latent], counts[...].astype(F32).astype(BF16), ACROSS) * mask

    def span_of(z):
        return pl.ds(pl.multiple_of(z * span, span), span)

    cl_line = []
    for i, z in enumerate(others):
        cl_line.append(
            remote(
                known_f.at[:, span_of(z)], cl_in.at[gene], ci_send.at[i], ci_recv.at[gene],
                {"gene": z},
            )
        )
        cl_line[-1].start()

    side[1].wait()
    g_out[1, lower] = g[1, core, lower] + g_pair[1, lower] + g_side[1]
    far.append(onward(1, lower, g_far.at[0, lower], gf_send.at[2], gf_recv.at[2], beside))
    side[0].wait()
    g_out[2, upper] = g[2, core, upper] + g_pair[2, upper] + g_side[0]
    far.append(onward(2, upper, g_far.at[1, upper], gf_send.at[3], gf_recv.at[3], above))
    p_forward(1)
    p_forward(2)
    pair[3].wait()
    total = g[3, core] + g_pair[3]
    for copy in far:
        copy.wait()
    total = total + g_far[0] + g_far[1]
    tall[0:rows] = total
    if rows < 128:
        tall[rows:128] = jnp.zeros((128 - rows, wide), F32)
    turned[...] = tall[...].T
    solve(turned, mine)
    out = []
    for d in range(1, n):
        out.append(
            remote(
                mine, b_all.at[gene, core, chip], b_send.at[d - 1], b_recv.at[d - 1],
                {"cell": lax.rem(cell + d, n)},
            )
        )
        out[-1].start()
    b_line = []
    for i, z in enumerate(others):
        b_line.append(
            remote(
                mine, b_all.at[gene, core, chip], bz_send.at[i], bz_recv.at[gene], {"gene": z}
            )
        )
        b_line[-1].start()
    b_all[gene, core, chip] = mine[...]

    total = known_f[:, span_of(gene)]
    for z in others:
        remote(cl_in.at[z], cl_in.at[z], ci_send.at[0], ci_recv.at[z], {"gene": near}).wait_recv()
        total = total + cl_in[z]
    cl_own[...] = total
    ca_line = []
    for i, z in enumerate(others):
        ca_line.append(
            remote(cl_own, cl_all.at[gene], ca_send.at[i], ca_recv.at[gene], {"gene": z})
        )
        ca_line[-1].start()
    cl_all[gene] = cl_own[...]

    p_pair = []
    for i, z in enumerate(others):
        for k in range(chips - 1):
            p_plane[i, k].wait()
        half = p_all.at[z, :, p_cols]
        p_pair.append(remote(half, half, pp_send.at[i], pp_recv.at[i], {"cell": partner}))
        p_pair[-1].start()
    for copy in out:
        copy.wait()

    def gather_betas(z):
        for o in range(n):
            b_cat[:, o * rows : (o + 1) * rows] = b_all[z, o % 2, o // 2, :, :rows]
        return b_cat[...]

    beta = gather_betas(gene)
    beta_ref[...] = beta
    beta_hi, beta_lo = split(beta)
    lhs_ref[...] = jnp.concatenate([beta_hi, beta_lo, beta_hi], axis=0).astype(F32).T.astype(BF16)
    b_plane = {}
    for i, z in enumerate(others):
        piece = b_all.at[z, core, chip]
        remote(piece, piece, bz_send.at[0], bz_recv.at[z], {"gene": near}).wait_recv()
        for k in range(chips - 1):
            b_plane[i, k] = remote(
                piece, piece, bx_send.at[i, k], bx_recv.at[i, k], {"cell": 2 * places[k] + core}
            )
            b_plane[i, k].start()

    lpair, lfar = [], []

    def hand_on(j):
        lpair[j].wait()
        l_out[j] = gl[j, core] + l_pair[j]
        lfar.append(
            remote(
                l_out.at[j], l_far.at[j], lf_send.at[j], lf_recv.at[j],
                {"cell": 2 * places[j] + core},
            )
        )
        lfar[-1].start()

    for j in range(chips):
        at = pl.ds(pl.multiple_of(places[j] * block, block), block)
        delta = mul(lhs_ref[at], rhs[0 : 3 * width], ACROSS)
        high, low = split(jnp.exp(lin[at] + delta))
        w_hi[at] = high
        w_lo[at] = low
        first = mul(high, f_all[...], ROWS_BY_ROWS)
        second = mul(low, f_all[0 : 2 * latent], ROWS_BY_ROWS)
        grad = known_c[at, 2 * width :] - first[:, :latent] - second[:, :latent]
        curv = first[:, latent : 2 * latent] + first[:, 2 * latent :] + second[:, latent:]
        gl[j] = jnp.concatenate([grad, curv], axis=1).reshape(2, rows, 2 * latent)
        lpair.append(
            remote(gl.at[j, 1 - core], l_pair.at[j], lp_send.at[j], lp_recv.at[j], {"cell": partner})
        )
        lpair[-1].start()
        if j > 0:
            hand_on(j - 1)

    def gene_sums(loads, high, low):
        first = mul(loads, high, ACROSS)
        second = mul(loads[0 : 2 * latent], low, ACROSS)
        grad = first[:latent] + second[:latent]
        curv = first[latent : 2 * latent] + first[2 * latent :] + second[latent:]
        return jnp.concatenate([grad, curv], axis=0)

    gf[...] = gene_sums(l_all[...], w_hi[...], w_lo[...])
    b_pair = []
    for i, z in enumerate(others):
        for k in range(chips - 1):
            b_plane[i, k].wait()
        half = b_all.at[z, core]
        b_pair.append(remote(half, half, bp_send.at[i], bp_recv.at[i], {"cell": partner}))
        b_pair[-1].start()
    lpair[-1].wait()
    total = gl[chips - 1, core] + l_pair[chips - 1]
    for j in range(chips - 1):
        lfar[j].wait()
        total = total + l_far[j]
    if rows < 128:
        total = jnp.concatenate([total, jnp.zeros((128 - rows, 2 * latent), F32)], axis=0)
    total = total.T
    my_l[...] = total[:latent] / jnp.sqrt(total[latent:] + 1.0)
    out_l = []
    for d in range(1, n):
        out_l.append(
            remote(
                my_l, their_l.at[cell], ol_send.at[d - 1], ol_recv.at[d - 1],
                {"cell": lax.rem(cell + d, n)},
            )
        )
        out_l[-1].start()
    their_l[cell] = my_l[...]
    for i, z in enumerate(others):
        p_pair[i].wait()
        b_pair[i].wait()
        next_hi, next_lo = split(p_all[z, 0:width] + gather_betas(z))
        shift_hi, shift_lo = split(p_all[z, width : width + BATCHES])
        wider = p_all[z, width + BATCHES :]
        one = wider.astype(BF16)
        two_hi, two_lo = split(wider * wider)
        lhs = jnp.concatenate([next_hi, next_lo, next_hi, shift_hi, shift_lo, one], axis=0)
        high, low = split(jnp.exp(mul(lhs, rhs[...], DOWN) + extra[0:1]))
        gf[...] += gene_sums(jnp.concatenate([one, two_hi, two_lo], axis=0), high, low)
    for z in others:
        remote(cl_own, cl_all.at[z], ca_send.at[0], ca_recv.at[z], {"gene": near}).wait_recv()
    for o in range(m):
        at = slice(o * span, (o + 1) * span)
        fs_ref[:, at] = (cl_all[o] - gf[:latent, at]) / (gf[latent:, at] + 1.0)
    for d in range(1, n):
        out_l[d - 1].wait()
    for o in range(n):
        ls_ref[:, o * rows : (o + 1) * rows] = their_l[o, :, :rows]
    for copy in p_line + cl_line + ca_line + b_line:
        copy.wait_send()


def pass_on(*refs):
    count = len(refs) // 2
    for source, target in zip(refs[:count], refs[count:]):
        target[...] = source[...]


def local_fused(
    n, m, counts, batch_id, live_cells, knot_bin, depth_frac, cell_covariates, coefficients,
    batch_effect, factors, loadings,
):
    genes, slots = counts.shape
    rows, span, latent = genes // n, slots // m, factors.shape[1]
    ncov = cell_covariates.shape[0]
    width = SPL + ncov
    wide = SPL * ncov + ncov * ncov * 3 // 4 + 2 * SPL + width
    chips = n // 2
    dma = pltpu.SemaphoreType.DMA
    shape = jax.ShapeDtypeStruct
    vmem = pltpu.VMEM

    def params(**kw):
        return pltpu.CompilerParams(vmem_limit_bytes=LIMIT, **kw)

    def stay(x):
        return pltpu.with_memory_space_constraint(x, pltpu.HBM)

    knot, frac, batch = (v.reshape(1, slots) for v in (knot_bin, depth_frac, batch_id))
    shapes = (shape((width, genes), F32), shape((latent, slots), F32), shape((latent, genes), F32))
    there = pl.BlockSpec(memory_space=pl.ANY)
    found = pl.pallas_call(
        functools.partial(all_kernel, n, m),
        out_shape=shapes,
        in_specs=[there, there, pl.BlockSpec(memory_space=pltpu.SMEM)] + [there] * 7,
        out_specs=(VM, VM, VM),
        scratch_shapes=[
            vmem((1, slots), jnp.int32),
            vmem((1, slots), jnp.int32),
            vmem((1, slots), F32),
            vmem((ncov, slots), F32),
            vmem((latent, slots), BF16),
            vmem((latent, genes), BF16),
            vmem((width + BATCHES + latent, genes), F32),
            vmem((m, width + BATCHES + latent, genes), F32),
            vmem((genes, slots), jnp.int32),
            vmem((genes, slots), F32),
            vmem((3 * width + 2 * BATCHES + latent, slots), BF16),
            vmem((wide, slots), BF16),
            vmem((wide, slots), BF16),
            vmem((2 * width + latent, slots), BF16),
            vmem((3 * latent, slots), BF16),
            vmem((3 * latent, genes), BF16),
            vmem((8, slots), F32),
            vmem((1, slots), F32),
            vmem((m - 1, 1, slots), F32),
            vmem((genes, 2 * width + latent), F32),
            vmem((latent, slots), F32),
            vmem((m, latent, span), F32),
            vmem((latent, span), F32),
            vmem((m, latent, span), F32),
            vmem((genes, slots), BF16),
            vmem((genes, slots), BF16),
            vmem((genes, 3 * width), BF16),
            vmem((chips, 2, rows, wide), F32),
            vmem((chips, rows, wide), F32),
            vmem((chips - 1, rows, wide), F32),
            vmem((2, rows // 2, wide), F32),
            vmem((2, rows, wide), F32),
            vmem((128, wide), F32),
            vmem((wide, 128), F32),
            vmem((width, 128), F32),
            vmem((m, 2, chips, width, 128), F32),
            vmem((width, genes), F32),
            vmem((chips, 2, rows, 2 * latent), F32),
            vmem((chips, rows, 2 * latent), F32),
            vmem((chips - 1, rows, 2 * latent), F32),
            vmem((chips - 1, rows, 2 * latent), F32),
            vmem((latent, 128), F32),
            vmem((n, latent, 128), F32),
            vmem((2 * latent, slots), F32),
            dma((n,)), dma((8,)), dma((m - 1,)), dma((m - 1,)),
            dma((m - 1,)), dma((m,)), dma((m - 1, chips - 1)), dma((m - 1, chips - 1)),
            dma((m - 1,)), dma((m - 1,)),
            dma((chips,)), dma((chips,)), dma((2,)), dma((2,)), dma((4,)), dma((4,)),
            dma((m - 1,)), dma((m,)), dma((m - 1,)), dma((m,)),
            dma((n - 1,)), dma((n - 1,)), dma((m - 1,)), dma((m,)),
            dma((m - 1, chips - 1)), dma((m - 1, chips - 1)), dma((m - 1,)), dma((m - 1,)),
            dma((chips,)), dma((chips,)), dma((chips - 1,)), dma((chips - 1,)),
            dma((n - 1,)), dma((n - 1,)),
        ],
        compiler_params=params(collective_id=0, has_side_effects=True),
        name="step",
    )(
        stay(counts), stay(batch), live_cells, stay(knot), stay(frac), stay(cell_covariates),
        stay(coefficients.T), stay(batch_effect.T), stay(factors.T), stay(loadings.T),
    )
    beta, fs, ls = pl.pallas_call(
        pass_on, out_shape=shapes, in_specs=[VM] * 3, out_specs=(VM, VM, VM),
        compiler_params=params(), name="finish",
    )(*found)
    return beta.T, fs.T, ls.T


def local(n, m, *args):
    counts, cov, factors = args[0], args[5], args[8]
    genes, slots = counts.shape
    fits = (
        n == 8
        and m == 4
        and genes % (16 * n) == 0
        and genes // n <= 128
        and slots % (128 * m) == 0
        and genes % 256 == 0
        and (SPL + cov.shape[0] + BATCHES + factors.shape[1]) % 32 == 0
        and cov.shape[0] == SPL
        and factors.shape[1] == 64
    )
    if fits:
        return local_fused(n, m, *args)
    return local_plain(*args)


def solution(mesh):
    placed = (
        P("gene", "cell"),
        P("cell"),
        P("cell"),
        P("cell"),
        P("cell"),
        P(None, "cell"),
        P("gene", None),
        P("gene", None),
        P("cell", None),
        P("gene", None),
    )
    return jax.shard_map(
        functools.partial(local, mesh.shape["cell"], mesh.shape["gene"]),
        mesh=mesh,
        in_specs=placed,
        out_specs=(P("gene", None), P("cell", None), P("gene", None)),
        check_vma=False,
    )
```

```python
import functools

import jax
import jax.numpy as jnp
from jax import lax
from jax.experimental import pallas as pl
from jax.experimental.pallas import tpu as pltpu
from jax.sharding import PartitionSpec as P

GENES = 3072
SPL = 16
BATCHES = 64


ridge_weight = 1.0


def design_rows(knot_bin, depth_frac, cell_covariates):
    levels = jnp.arange(SPL, dtype=jnp.int32)[:, None]
    fraction = depth_frac[None, :]
    hat_basis = jnp.where(levels == knot_bin[None, :], 1.0 - fraction, 0.0)
    hat_basis = hat_basis + jnp.where(levels == knot_bin[None, :] + 1, fraction, 0.0)
    return jnp.concatenate([hat_basis, cell_covariates], axis=0)


def newton_solve(gram_flat, score):
    columns = score.shape[-1]
    identity = jnp.eye(columns, dtype=gram_flat.dtype)
    system = gram_flat.reshape(-1, columns, columns) + ridge_weight * identity
    factor_lower = jnp.linalg.cholesky(system)
    middle = jax.scipy.linalg.solve_triangular(factor_lower, score[..., None], lower=True)
    return jax.scipy.linalg.solve_triangular(factor_lower, middle, lower=True, trans=1)[..., 0]


def local_plain(
    counts,
    batch_id,
    live_cells,
    knot_bin,
    depth_frac,
    cell_covariates,
    coefficients,
    batch_effect,
    factors,
    loadings,
):
    highest = lax.Precision.HIGHEST
    contract = (((1,), (1,)), ((), ()))
    observed = counts.astype(jnp.float32)
    totals = lax.psum(jnp.sum(observed, axis=0), "gene")
    offset = jnp.log((1.0 + totals) / GENES)
    slot_count = observed.shape[1]
    live_mask = (jnp.arange(slot_count, dtype=jnp.int32) < live_cells[0]).astype(jnp.float32)
    design = design_rows(knot_bin, depth_frac, cell_covariates)
    columns = design.shape[0]
    onehot = (jnp.arange(BATCHES, dtype=jnp.int32)[:, None] == batch_id[None, :]).astype(
        jnp.float32
    )
    stacked = jnp.concatenate([design, onehot], axis=0)
    linear = jnp.dot(
        jnp.concatenate([coefficients, batch_effect], axis=1), stacked, precision=highest
    )
    latent = lax.dot_general(loadings, factors, contract, preferred_element_type=jnp.float32)
    linear_pred = offset[None, :] + linear + latent
    expected = jnp.exp(linear_pred)
    weight = expected * live_mask
    residual = (observed - expected) * live_mask
    pairs = (design[:, None, :] * design[None, :, :]).reshape(columns * columns, slot_count)
    gram_part = lax.dot_general(weight, pairs, contract, precision=highest)
    score_part = lax.dot_general(residual, design, contract, precision=highest)
    gram_share, score_share = (
        lax.psum_scatter(gram_part, "cell", scatter_dimension=0, tiled=True),
        lax.psum_scatter(score_part, "cell", scatter_dimension=0, tiled=True),
    )
    step_share = newton_solve(gram_share, score_share)
    beta_step = lax.all_gather(step_share, "cell", axis=0, tiled=True)
    expected_next = jnp.exp(linear_pred + jnp.dot(beta_step, design, precision=highest))
    weight_next = expected_next * live_mask
    residual_next = (observed - expected_next) * live_mask
    factors_wide = factors.astype(jnp.float32)
    loads_wide = loadings.astype(jnp.float32)
    grad_load = jnp.dot(residual_next, factors_wide, precision=highest)
    curv_load = jnp.dot(weight_next, factors_wide * factors_wide, precision=highest)
    back = (((0,), (0,)), ((), ()))
    grad_fact = lax.dot_general(residual_next, loads_wide, back, precision=highest)
    curv_fact = lax.dot_general(weight_next, loads_wide * loads_wide, back, precision=highest)
    grad_load, curv_load = lax.psum((grad_load, curv_load), "cell")
    grad_fact, curv_fact = lax.psum((grad_fact, curv_fact), "gene")
    factor_step = grad_fact / (curv_fact + 1.0)
    loading_score = grad_load / jnp.sqrt(curv_load + 1.0)
    return (beta_step, factor_step, loading_score)


MESH = pl.DeviceIdType.MESH
F32, BF16 = jnp.float32, jnp.bfloat16
VM = pl.BlockSpec(memory_space=pltpu.VMEM)
ROWS_BY_ROWS = (((1,), (1,)), ((), ()))
ACROSS = (((1,), (0,)), ((), ()))
DOWN = (((0,), (0,)), ((), ()))
LIMIT = 40 * 1024 * 1024


def split(x):
    high = x.astype(BF16)
    return high, (x - high.astype(F32)).astype(BF16)


def mul(a, b, dims):
    return lax.dot_general(a, b, dims, preferred_element_type=F32)


def remote(src, dst, send, recv, where):
    return pltpu.make_async_remote_copy(
        src_ref=src, dst_ref=dst, send_sem=send, recv_sem=recv, device_id=where, device_id_type=MESH
    )


def meet_signal(groups):
    barrier = pltpu.get_barrier_semaphore()
    count = 0
    for axis, n in groups:
        me = lax.axis_index(axis)
        for d in range(1, n):
            pl.semaphore_signal(
                barrier, inc=1, device_id={axis: lax.rem(me + d, n)}, device_id_type=MESH
            )
        count += n - 1
    return lambda: pl.semaphore_wait(barrier, count)


def design_of(knot_ref, frac_ref, cov_ref):
    slots = knot_ref.shape[1]
    levels = lax.broadcasted_iota(jnp.int32, (SPL, slots), 0)
    knot, frac = knot_ref[...], frac_ref[...]
    hats = jnp.where(levels == knot, 1.0 - frac, 0.0)
    hats = hats + jnp.where(levels == knot + 1, frac, 0.0)
    return hats, cov_ref[...]


def build_pairs(hats, cov, pair_hi, pair_lo):
    slots = hats.shape[1]
    ncov = cov.shape[0]
    half = ncov // 2

    def put(at, block):
        high, low = split(block)
        pair_hi[at : at + block.shape[0]] = high
        pair_lo[at : at + block.shape[0]] = low

    at = 0
    for p in range(SPL):
        put(at, hats[p : p + 1] * cov)
        at += ncov
    for i in range(half):
        put(at, cov[i : i + 1] * cov)
        at += ncov
    for i in range(half, ncov, 2):
        put(
            at,
            jnp.concatenate(
                [cov[i : i + 1] * cov[half:], cov[i + 1 : i + 2] * cov[half:]], axis=0
            ),
        )
        at += ncov
    put(at, hats * hats)
    at += SPL
    later = jnp.concatenate([hats[1:], jnp.zeros((1, slots), F32)], axis=0)
    put(at, hats * later)
    at += SPL
    put(at, jnp.zeros((SPL + ncov, slots), F32))


def solve(g, x):
    half = SPL // 2
    cov_at, low_at, hat_at = SPL * SPL, SPL * SPL + half * SPL, SPL * SPL + half * SPL + half * half
    off_at, score_at = hat_at + SPL, hat_at + 2 * SPL
    spot = lax.broadcasted_iota(jnp.int32, (half, g.shape[1]), 0)

    def one(block, i):
        return block[i : i + 1]

    lo = {}
    hi = {}
    for i in range(SPL):
        unit = jnp.where(spot == i % half, ridge_weight, 0.0)
        if i < half:
            lo[i] = g[cov_at + i * SPL : cov_at + i * SPL + half] + unit
            hi[i] = g[cov_at + i * SPL + half : cov_at + (i + 1) * SPL]
        else:
            hi[i] = g[low_at + (i - half) * half : low_at + (i - half + 1) * half] + unit
    b_lo = g[score_at + SPL : score_at + SPL + half]
    b_hi = g[score_at + SPL + half : score_at + 2 * SPL]
    sums_lo, sums_hi = g[0:half], g[half:SPL]
    for p in range(1, SPL):
        sums_lo = sums_lo + g[p * SPL : p * SPL + half]
        sums_hi = sums_hi + g[p * SPL + half : (p + 1) * SPL]
    b_lo, b_hi = b_lo - sums_lo, b_hi - sums_hi
    pivot_inv, edge, side_lo, side_hi, rest = [], [], [], [], []
    for p in range(SPL):
        own = g[hat_at + p : hat_at + p + 1]
        after = g[off_at + p : off_at + p + 1]
        d = own + ridge_weight
        u_lo = g[p * SPL : p * SPL + half]
        u_hi = g[p * SPL + half : (p + 1) * SPL]
        b = g[score_at + p : score_at + p + 1] - own - after
        if p > 0:
            b = b - edge[-1]
            ratio = edge[-1] * pivot_inv[-1]
            d = d - ratio * edge[-1]
            u_lo = u_lo - ratio * side_lo[-1]
            u_hi = u_hi - ratio * side_hi[-1]
            b = b - ratio * rest[-1]
        inv = 1.0 / d
        pivot_inv.append(inv)
        edge.append(after)
        side_lo.append(u_lo)
        side_hi.append(u_hi)
        rest.append(b)
        scaled_lo, scaled_hi = u_lo * inv, u_hi * inv
        b_lo = b_lo - scaled_lo * b
        b_hi = b_hi - scaled_hi * b
        for i in range(SPL):
            if i < half:
                f = one(scaled_lo, i)
                lo[i] = lo[i] - f * u_lo
            else:
                f = one(scaled_hi, i - half)
            hi[i] = hi[i] - f * u_hi
    c_inv, c_rest = [], []
    for j in range(SPL):
        if j < half:
            inv = 1.0 / one(lo[j], j)
            b = one(b_lo, j)
            s_lo = lo[j] * inv
            b_lo = b_lo - s_lo * b
        else:
            inv = 1.0 / one(hi[j], j - half)
            b = one(b_hi, j - half)
        s_hi = hi[j] * inv
        b_hi = b_hi - s_hi * b
        c_inv.append(inv)
        c_rest.append(b)
        for i in range(j + 1, SPL):
            if i < half:
                f = one(s_lo, i)
                lo[i] = lo[i] - f * lo[j]
            else:
                f = one(s_hi, i - half)
            hi[i] = hi[i] - f * hi[j]
    for j in reversed(range(SPL)):
        found = c_rest[j] * c_inv[j]
        x[SPL + j : SPL + j + 1] = found
        for i in range(j):
            c_rest[i] = c_rest[i] - (one(hi[i], j - half) if j >= half else one(lo[i], j)) * found
    x_lo, x_hi = x[SPL : SPL + half], x[SPL + half : 2 * SPL]
    after = None
    for p in reversed(range(SPL)):
        gone = jnp.sum(side_lo[p] * x_lo + side_hi[p] * x_hi, axis=0, keepdims=True)
        b = rest[p] - gone
        if after is not None:
            b = b - edge[p] * after
        after = b * pivot_inv[p]
        x[p : p + 1] = after


def pack(block, full):
    height, lanes = block.shape
    kept = height * full // lanes
    rest, part = block[kept:], lanes - full
    found = [
        pltpu.roll(rest, lanes - part - part * k, 1)[:, full:] for k in range(full // part)
    ]
    return jnp.concatenate([block[:kept, :full], jnp.concatenate(found, axis=0)], axis=1)


def unpack(target, o, full, ref):
    kept, lanes = ref.shape
    part = lanes - full
    more = kept * part // full
    target[:kept, o * full : (o + 1) * full] = ref[:, :full]
    for k in range(full // part):
        at = o * full + k * part
        target[kept:, at : at + part] = ref[k * more : (k + 1) * more, full:]


def all_kernel(
    n, m, counts_hbm, batch_hbm, live_ref, knot_hbm, frac_hbm, cov_hbm, coef_hbm, shift_hbm,
    factors_hbm, loads_hbm, beta_ref, fs_ref, ls_ref,
    batch_ref, knot_ref, frac_ref, cov_ref, factors_ref, loads_ref, p_own, p_all,
    counts, lin, rhs, pair_hi, pair_lo, tally, f_all, l_all, extra, tot_out, tot_in, known_c, known_f,
    cl_in, cl_own, cl_all, w_hi, w_lo, lhs_ref, g, g_pair, g_out, g_side, g_far, tall, turned, mine,
    packed, b_all, b_cat, gl, l_pair, l_out, l_far, my_l, their_l, gf,
    c_sem, i_sem, t_send, t_recv, pz_send, pz_recv, px_send, px_recv, pp_send, pp_recv,
    gp_send, gp_recv, gs_send, gs_recv, gf_send, gf_recv, ci_send, ci_recv, ca_send, ca_recv,
    b_send, b_recv, bz_send, bz_recv, bx_send, bx_recv, bp_send, bp_recv,
    lp_send, lp_recv, lf_send, lf_recv, ol_send, ol_recv,
):
    cell, gene = lax.axis_index("cell"), lax.axis_index("gene")
    core, chip = lax.rem(cell, 2), cell // 2
    chips = n // 2
    genes, slots = counts.shape
    block = genes // chips
    rows = genes // n
    latent = loads_ref.shape[0]
    span = slots // m
    width = SPL + cov_hbm.shape[0]
    tall_p = p_own.shape[0]
    coef_ref, shift_ref = p_own.at[0:width], p_own.at[width : width + BATCHES]
    arrive = meet_signal((("cell", n), ("gene", m)))
    loads_in = []
    for i in range(n):
        at = pl.ds(i * rows, rows)
        loads_in.append(pltpu.make_async_copy(counts_hbm.at[at], counts.at[at], c_sem.at[i]))
        loads_in[-1].start()
    small = []
    for i, (source, target) in enumerate(
        (
            (batch_hbm, batch_ref), (knot_hbm, knot_ref), (frac_hbm, frac_ref), (cov_hbm, cov_ref),
            (coef_hbm, coef_ref), (shift_hbm, shift_ref), (factors_hbm, factors_ref),
            (loads_hbm, loads_ref),
        )
    ):
        small.append(pltpu.make_async_copy(source, target, i_sem.at[i]))
        small[-1].start()
    part = None
    for i in range(n):
        loads_in[i].wait()
        piece = jnp.sum(counts[i * rows : (i + 1) * rows].reshape(rows // 8, 8, slots), axis=0)
        part = piece if part is None else part + piece
    tot_out[...] = jnp.sum(part, axis=0, keepdims=True).astype(F32)
    for copy in small:
        copy.wait()
    p_own[width + BATCHES :] = loads_ref[...].astype(F32)
    arrive()
    tot = []
    for d in range(1, m):
        tot.append(
            remote(
                tot_out, tot_in.at[d - 1], t_send.at[d - 1], t_recv.at[d - 1],
                {"gene": lax.rem(gene + d, m)},
            )
        )
        tot[-1].start()

    near = gene + 1 - 2 * lax.rem(gene, 2)
    others = [near, m - 1 - gene, lax.rem(gene + 2, m)]
    beside, above = chip + 1 - 2 * lax.rem(chip, 2), lax.rem(chip + 2, chips)
    places = [chips - 1 - chip, beside, above, chip]
    partner = cell + 1 - 2 * core
    deep, broad = tall_p // 2, genes // 2
    p_cols = pl.ds(pl.multiple_of(core * broad, broad), broad)
    p_rows = [
        pl.ds(0, tall_p),
        pl.ds(pl.multiple_of(lax.rem(chip, 2) * deep, deep), deep),
        pl.ds(pl.multiple_of(chip // 2 * deep, deep), deep),
    ]
    p_line = {}
    for i in (1, 2, 0):
        p_line[i] = remote(
            p_own.at[p_rows[i], p_cols], p_all.at[gene, p_rows[i], p_cols], pz_send.at[i],
            pz_recv.at[i], {"gene": others[i]},
        )
    p_plane = {}

    def p_forward(i, place):
        p_line[i].wait()
        piece = p_all.at[others[i], p_rows[i], p_cols]
        p_plane[i] = remote(
            piece, piece, px_send.at[i - 1], px_recv.at[i - 1], {"cell": 2 * place + core}
        )
        p_plane[i].start()

    hats, cov = design_of(knot_ref, frac_ref, cov_ref)
    design_hi, design_lo = split(jnp.concatenate([hats, cov], axis=0))
    hot = lax.broadcasted_iota(jnp.int32, (BATCHES, slots), 0) == batch_ref[...]
    hot = jnp.where(hot, 1.0, 0.0).astype(BF16)
    rhs[0:width] = design_hi
    rhs[width : 2 * width] = design_hi
    rhs[2 * width : 3 * width] = design_lo
    rhs[3 * width : 3 * width + BATCHES] = hot
    rhs[3 * width + BATCHES : 3 * width + 2 * BATCHES] = hot
    rhs[3 * width + 2 * BATCHES :] = factors_ref[...]
    coef_hi, coef_lo = split(coef_ref[...])
    shift_hi, shift_lo = split(shift_ref[...])
    lhs = jnp.concatenate([coef_hi, coef_lo, coef_hi, shift_hi, shift_lo, loads_ref[...]], axis=0)
    lin[...] = mul(lhs, rhs[...], DOWN)
    build_pairs(hats, cov, pair_hi, pair_lo)
    live = lax.broadcasted_iota(jnp.int32, (1, slots), 1) < live_ref[0]
    mask = jnp.where(live, 1.0, 0.0)
    mask_bf = mask.astype(BF16)
    factors_live = factors_ref[...].astype(F32) * mask
    tally[0:width] = design_hi * mask_bf
    tally[width : 2 * width] = design_lo * mask_bf
    tally[2 * width :] = factors_live.astype(BF16)
    known_c[...] = mul(counts[...].astype(F32).astype(BF16), tally[...], ROWS_BY_ROWS)

    total = tot_out[...]
    for d in range(1, m):
        tot[d - 1].wait()
        total = total + tot_in[d - 1]
    extra[0:1] = jnp.where(live, jnp.log((1.0 + total) / GENES), -1e30)
    for i in (1, 2, 0):
        p_line[i].start()

    wide = g.shape[3]
    cut = rows // 2
    upper, lower = slice(0, cut), slice(cut, rows)

    def gram_chunk(j):
        at = pl.ds(pl.multiple_of(places[j] * block, block), block)
        linear = lin[at] + extra[0:1]
        lin[at] = linear
        high, low = split(jnp.exp(linear))
        both = mul(jnp.concatenate([high, low], axis=0), pair_hi[...], ROWS_BY_ROWS)
        gram = both[:block] + both[block:] + mul(high, pair_lo[...], ROWS_BY_ROWS)
        counted = known_c[at, 0:width] + known_c[at, width : 2 * width]
        g[j, :, :, : wide - width] = gram[:, : wide - width].reshape(2, rows, wide - width)
        g[j, :, :, wide - width :] = counted.reshape(2, rows, width)
        copy = remote(
            g.at[j, 1 - core], g_pair.at[j], gp_send.at[j], gp_recv.at[j], {"cell": partner}
        )
        copy.start()
        return copy

    def onward(j, part, target, send, recv, place):
        copy = remote(g_out.at[j, part], target, send, recv, {"cell": 2 * place + core})
        copy.start()
        return copy

    pair = [gram_chunk(0), gram_chunk(1)]
    pair[0].wait()
    g_out[0] = g[0, core] + g_pair[0]
    side = [
        onward(0, upper, g_side.at[0], gs_send.at[0], gs_recv.at[0], beside),
        onward(0, lower, g_side.at[1], gs_send.at[1], gs_recv.at[1], above),
    ]
    pair.append(gram_chunk(2))
    pair[1].wait()
    g_out[1, upper] = g[1, core, upper] + g_pair[1, upper]
    far = [onward(1, upper, g_far.at[0, upper], gf_send.at[0], gf_recv.at[0], beside)]
    pair.append(gram_chunk(3))
    pair[2].wait()
    g_out[2, lower] = g[2, core, lower] + g_pair[2, lower]
    far.append(onward(2, lower, g_far.at[1, lower], gf_send.at[1], gf_recv.at[1], above))

    f_hi, f_lo = split(factors_live * factors_live)
    f_all[0:latent] = tally[2 * width :]
    f_all[latent : 2 * latent] = f_hi
    f_all[2 * latent :] = f_lo
    loads_wide = loads_ref[...].astype(F32)
    l_hi, l_lo = split(loads_wide * loads_wide)
    l_all[0:latent] = loads_ref[...]
    l_all[latent : 2 * latent] = l_hi
    l_all[2 * latent :] = l_lo

    known_f[...] = mul(l_all[0:latent], counts[...].astype(F32).astype(BF16), ACROSS) * mask

    def span_of(z):
        return pl.ds(pl.multiple_of(z * span, span), span)

    cl_line = []
    for i, z in enumerate(others):
        cl_line.append(
            remote(
                known_f.at[:, span_of(z)], cl_in.at[gene], ci_send.at[i], ci_recv.at[gene],
                {"gene": z},
            )
        )
        cl_line[-1].start()

    side[1].wait()
    g_out[1, lower] = g[1, core, lower] + g_pair[1, lower] + g_side[1]
    far.append(onward(1, lower, g_far.at[0, lower], gf_send.at[2], gf_recv.at[2], beside))
    side[0].wait()
    g_out[2, upper] = g[2, core, upper] + g_pair[2, upper] + g_side[0]
    far.append(onward(2, upper, g_far.at[1, upper], gf_send.at[3], gf_recv.at[3], above))
    pair[3].wait()
    total = g[3, core] + g_pair[3]
    for copy in far:
        copy.wait()
    total = total + g_far[0] + g_far[1]
    tall[0:rows] = total
    if rows < 128:
        tall[rows:128] = jnp.zeros((128 - rows, wide), F32)
    turned[...] = tall[...].T
    solve(turned, mine)
    packed[...] = pack(mine[...], rows)
    b_line = []
    for i, z in enumerate(others):
        b_line.append(
            remote(packed, b_all.at[gene, core, chip], bz_send.at[i], bz_recv.at[i], {"gene": z})
        )
        b_line[-1].start()
    out = []
    for d in range(1, n):
        out.append(
            remote(
                packed, b_all.at[gene, core, chip], b_send.at[d - 1], b_recv.at[d - 1],
                {"cell": lax.rem(cell + d, n)},
            )
        )
        out[-1].start()
    b_all[gene, core, chip] = packed[...]

    b_plane = {}

    def b_forward(i):
        b_line[i].wait()
        piece = b_all.at[others[i], core, chip]
        for k in range(chips - 1):
            b_plane[i, k] = remote(
                piece, piece, bx_send.at[i, k], bx_recv.at[i, k], {"cell": 2 * places[k] + core}
            )
            b_plane[i, k].start()

    b_pair = []

    def b_swap(i):
        for k in range(chips - 1):
            b_plane[i, k].wait()
        half = b_all.at[others[i], core]
        b_pair.append(remote(half, half, bp_send.at[i], bp_recv.at[i], {"cell": partner}))
        b_pair[-1].start()

    b_forward(0)
    p_forward(1, beside)
    p_forward(2, above)
    for copy in out:
        copy.wait()

    def gather_betas(z):
        for o in range(n):
            unpack(b_cat, o, rows, b_all.at[z, o % 2, o // 2])
        return b_cat[...]

    beta = gather_betas(gene)
    beta_ref[...] = beta
    beta_hi, beta_lo = split(beta)
    lhs_ref[...] = jnp.concatenate([beta_hi, beta_lo, beta_hi], axis=0).astype(F32).T.astype(BF16)
    b_forward(1)
    b_forward(2)

    lpair, lfar = [], []

    def hand_on(j):
        lpair[j].wait()
        l_out[j] = gl[j, core] + l_pair[j]
        lfar.append(
            remote(
                l_out.at[j], l_far.at[j], lf_send.at[j], lf_recv.at[j],
                {"cell": 2 * places[j] + core},
            )
        )
        lfar[-1].start()

    for j in range(chips):
        at = pl.ds(pl.multiple_of(places[j] * block, block), block)
        delta = mul(lhs_ref[at], rhs[0 : 3 * width], ACROSS)
        high, low = split(jnp.exp(lin[at] + delta))
        w_hi[at] = high
        w_lo[at] = low
        first = mul(high, f_all[...], ROWS_BY_ROWS)
        second = mul(low, f_all[0 : 2 * latent], ROWS_BY_ROWS)
        grad = known_c[at, 2 * width :] - first[:, :latent] - second[:, :latent]
        curv = first[:, latent : 2 * latent] + first[:, 2 * latent :] + second[:, latent:]
        gl[j] = jnp.concatenate([grad, curv], axis=1).reshape(2, rows, 2 * latent)
        lpair.append(
            remote(gl.at[j, 1 - core], l_pair.at[j], lp_send.at[j], lp_recv.at[j], {"cell": partner})
        )
        lpair[-1].start()
        if j > 0:
            hand_on(j - 1)

    def gene_sums(loads, high, low):
        first = mul(loads, high, ACROSS)
        second = mul(loads[0 : 2 * latent], low, ACROSS)
        grad = first[:latent] + second[:latent]
        curv = first[latent : 2 * latent] + first[2 * latent :] + second[latent:]
        return jnp.concatenate([grad, curv], axis=0)

    p_pair = []
    p_line[0].wait()
    p_plane[1].wait()
    p_plane[2].wait()
    for i, z in enumerate(others):
        half = p_all.at[z, :, p_cols]
        p_pair.append(remote(half, half, pp_send.at[i], pp_recv.at[i], {"cell": partner}))
        p_pair[-1].start()
    b_swap(0)
    gf[...] = gene_sums(l_all[...], w_hi[...], w_lo[...])

    def other_genes(i):
        z = others[i]
        p_pair[i].wait()
        b_pair[i].wait()
        next_hi, next_lo = split(p_all[z, 0:width] + gather_betas(z))
        shift_hi, shift_lo = split(p_all[z, width : width + BATCHES])
        wider = p_all[z, width + BATCHES :]
        one = wider.astype(BF16)
        two_hi, two_lo = split(wider * wider)
        lhs = jnp.concatenate([next_hi, next_lo, next_hi, shift_hi, shift_lo, one], axis=0)
        high, low = split(jnp.exp(mul(lhs, rhs[...], DOWN) + extra[0:1]))
        gf[...] += gene_sums(jnp.concatenate([one, two_hi, two_lo], axis=0), high, low)

    total = known_f[:, span_of(gene)]
    for z in others:
        remote(cl_in.at[z], cl_in.at[z], ci_send.at[0], ci_recv.at[z], {"gene": near}).wait_recv()
        total = total + cl_in[z]
    cl_own[...] = total
    ca_line = []
    for i, z in enumerate(others):
        ca_line.append(
            remote(cl_own, cl_all.at[gene], ca_send.at[i], ca_recv.at[gene], {"gene": z})
        )
        ca_line[-1].start()
    cl_all[gene] = cl_own[...]

    lpair[-1].wait()
    total = gl[chips - 1, core] + l_pair[chips - 1]
    b_swap(1)
    b_swap(2)
    other_genes(0)
    for j in range(chips - 1):
        lfar[j].wait()
        total = total + l_far[j]
    if rows < 128:
        total = jnp.concatenate([total, jnp.zeros((128 - rows, 2 * latent), F32)], axis=0)
    total = total.T
    my_l[...] = pack(total[:latent] / jnp.sqrt(total[latent:] + 1.0), rows)
    out_l = []
    for d in range(1, n):
        out_l.append(
            remote(
                my_l, their_l.at[cell], ol_send.at[d - 1], ol_recv.at[d - 1],
                {"cell": lax.rem(cell + d, n)},
            )
        )
        out_l[-1].start()
    their_l[cell] = my_l[...]
    other_genes(1)
    other_genes(2)
    for z in others:
        remote(cl_own, cl_all.at[z], ca_send.at[0], ca_recv.at[z], {"gene": near}).wait_recv()
    for o in range(m):
        at = slice(o * span, (o + 1) * span)
        fs_ref[:, at] = (cl_all[o] - gf[:latent, at]) / (gf[latent:, at] + 1.0)
    for d in range(1, n):
        out_l[d - 1].wait()
    for o in range(n):
        unpack(ls_ref, o, rows, their_l.at[o])
    for copy in cl_line + ca_line:
        copy.wait_send()


def pass_on(*refs):
    count = len(refs) // 2
    for source, target in zip(refs[:count], refs[count:]):
        target[...] = source[...]


def local_fused(
    n, m, counts, batch_id, live_cells, knot_bin, depth_frac, cell_covariates, coefficients,
    batch_effect, factors, loadings,
):
    genes, slots = counts.shape
    rows, span, latent = genes // n, slots // m, factors.shape[1]
    ncov = cell_covariates.shape[0]
    width = SPL + ncov
    wide = SPL * ncov + ncov * ncov * 3 // 4 + 2 * SPL + width
    chips = n // 2
    dma = pltpu.SemaphoreType.DMA
    shape = jax.ShapeDtypeStruct
    vmem = pltpu.VMEM

    def params(**kw):
        return pltpu.CompilerParams(vmem_limit_bytes=LIMIT, **kw)

    def stay(x):
        return pltpu.with_memory_space_constraint(x, pltpu.HBM)

    knot, frac, batch = (v.reshape(1, slots) for v in (knot_bin, depth_frac, batch_id))
    shapes = (shape((width, genes), F32), shape((latent, slots), F32), shape((latent, genes), F32))
    there = pl.BlockSpec(memory_space=pl.ANY)
    found = pl.pallas_call(
        functools.partial(all_kernel, n, m),
        out_shape=shapes,
        in_specs=[there, there, pl.BlockSpec(memory_space=pltpu.SMEM)] + [there] * 7,
        out_specs=(VM, VM, VM),
        scratch_shapes=[
            vmem((1, slots), jnp.int32),
            vmem((1, slots), jnp.int32),
            vmem((1, slots), F32),
            vmem((ncov, slots), F32),
            vmem((latent, slots), BF16),
            vmem((latent, genes), BF16),
            vmem((width + BATCHES + latent, genes), F32),
            vmem((m, width + BATCHES + latent, genes), F32),
            vmem((genes, slots), jnp.int32),
            vmem((genes, slots), F32),
            vmem((3 * width + 2 * BATCHES + latent, slots), BF16),
            vmem((wide, slots), BF16),
            vmem((wide, slots), BF16),
            vmem((2 * width + latent, slots), BF16),
            vmem((3 * latent, slots), BF16),
            vmem((3 * latent, genes), BF16),
            vmem((8, slots), F32),
            vmem((1, slots), F32),
            vmem((m - 1, 1, slots), F32),
            vmem((genes, 2 * width + latent), F32),
            vmem((latent, slots), F32),
            vmem((m, latent, span), F32),
            vmem((latent, span), F32),
            vmem((m, latent, span), F32),
            vmem((genes, slots), BF16),
            vmem((genes, slots), BF16),
            vmem((genes, 3 * width), BF16),
            vmem((chips, 2, rows, wide), F32),
            vmem((chips, rows, wide), F32),
            vmem((chips - 1, rows, wide), F32),
            vmem((2, rows // 2, wide), F32),
            vmem((2, rows, wide), F32),
            vmem((128, wide), F32),
            vmem((wide, 128), F32),
            vmem((width, 128), F32),
            vmem((width * rows // 128, 128), F32),
            vmem((m, 2, chips, width * rows // 128, 128), F32),
            vmem((width, genes), F32),
            vmem((chips, 2, rows, 2 * latent), F32),
            vmem((chips, rows, 2 * latent), F32),
            vmem((chips - 1, rows, 2 * latent), F32),
            vmem((chips - 1, rows, 2 * latent), F32),
            vmem((latent * rows // 128, 128), F32),
            vmem((n, latent * rows // 128, 128), F32),
            vmem((2 * latent, slots), F32),
            dma((n,)), dma((8,)), dma((m - 1,)), dma((m - 1,)),
            dma((m - 1,)), dma((m - 1,)), dma((2,)), dma((2,)),
            dma((m - 1,)), dma((m - 1,)),
            dma((chips,)), dma((chips,)), dma((2,)), dma((2,)), dma((4,)), dma((4,)),
            dma((m - 1,)), dma((m,)), dma((m - 1,)), dma((m,)),
            dma((n - 1,)), dma((n - 1,)), dma((m - 1,)), dma((m - 1,)),
            dma((m - 1, chips - 1)), dma((m - 1, chips - 1)), dma((m - 1,)), dma((m - 1,)),
            dma((chips,)), dma((chips,)), dma((chips - 1,)), dma((chips - 1,)),
            dma((n - 1,)), dma((n - 1,)),
        ],
        compiler_params=params(collective_id=0, has_side_effects=True),
        name="step",
    )(
        stay(counts), stay(batch), live_cells, stay(knot), stay(frac), stay(cell_covariates),
        stay(coefficients.T), stay(batch_effect.T), stay(factors.T), stay(loadings.T),
    )
    beta, fs, ls = pl.pallas_call(
        pass_on, out_shape=shapes, in_specs=[VM] * 3, out_specs=(VM, VM, VM),
        compiler_params=params(), name="finish",
    )(*found)
    return beta.T, fs.T, ls.T


def local(n, m, *args):
    counts, cov, factors = args[0], args[5], args[8]
    genes, slots = counts.shape
    fits = (
        n == 8
        and m == 4
        and genes % (16 * n) == 0
        and genes // n == 96
        and slots % (128 * m) == 0
        and genes % 256 == 0
        and (SPL + cov.shape[0] + BATCHES + factors.shape[1]) % 16 == 0
        and cov.shape[0] == SPL
        and factors.shape[1] == 64
    )
    if fits:
        return local_fused(n, m, *args)
    return local_plain(*args)


def solution(mesh):
    placed = (
        P("gene", "cell"),
        P("cell"),
        P("cell"),
        P("cell"),
        P("cell"),
        P(None, "cell"),
        P("gene", None),
        P("gene", None),
        P("cell", None),
        P("gene", None),
    )
    return jax.shard_map(
        functools.partial(local, mesh.shape["cell"], mesh.shape["gene"]),
        mesh=mesh,
        in_specs=placed,
        out_specs=(P("gene", None), P("cell", None), P("gene", None)),
        check_vma=False,
    )
```

```python
import functools

import jax
import jax.numpy as jnp
from jax import lax
from jax.experimental import pallas as pl
from jax.experimental.pallas import tpu as pltpu
from jax.sharding import PartitionSpec as P

GENES = 3072
SPL = 16
BATCHES = 64


ridge_weight = 1.0


def design_rows(knot_bin, depth_frac, cell_covariates):
    levels = jnp.arange(SPL, dtype=jnp.int32)[:, None]
    fraction = depth_frac[None, :]
    hat_basis = jnp.where(levels == knot_bin[None, :], 1.0 - fraction, 0.0)
    hat_basis = hat_basis + jnp.where(levels == knot_bin[None, :] + 1, fraction, 0.0)
    return jnp.concatenate([hat_basis, cell_covariates], axis=0)


def newton_solve(gram_flat, score):
    columns = score.shape[-1]
    identity = jnp.eye(columns, dtype=gram_flat.dtype)
    system = gram_flat.reshape(-1, columns, columns) + ridge_weight * identity
    factor_lower = jnp.linalg.cholesky(system)
    middle = jax.scipy.linalg.solve_triangular(factor_lower, score[..., None], lower=True)
    return jax.scipy.linalg.solve_triangular(factor_lower, middle, lower=True, trans=1)[..., 0]


def local_plain(
    counts,
    batch_id,
    live_cells,
    knot_bin,
    depth_frac,
    cell_covariates,
    coefficients,
    batch_effect,
    factors,
    loadings,
):
    highest = lax.Precision.HIGHEST
    contract = (((1,), (1,)), ((), ()))
    observed = counts.astype(jnp.float32)
    totals = lax.psum(jnp.sum(observed, axis=0), "gene")
    offset = jnp.log((1.0 + totals) / GENES)
    slot_count = observed.shape[1]
    live_mask = (jnp.arange(slot_count, dtype=jnp.int32) < live_cells[0]).astype(jnp.float32)
    design = design_rows(knot_bin, depth_frac, cell_covariates)
    columns = design.shape[0]
    onehot = (jnp.arange(BATCHES, dtype=jnp.int32)[:, None] == batch_id[None, :]).astype(
        jnp.float32
    )
    stacked = jnp.concatenate([design, onehot], axis=0)
    linear = jnp.dot(
        jnp.concatenate([coefficients, batch_effect], axis=1), stacked, precision=highest
    )
    latent = lax.dot_general(loadings, factors, contract, preferred_element_type=jnp.float32)
    linear_pred = offset[None, :] + linear + latent
    expected = jnp.exp(linear_pred)
    weight = expected * live_mask
    residual = (observed - expected) * live_mask
    pairs = (design[:, None, :] * design[None, :, :]).reshape(columns * columns, slot_count)
    gram_part = lax.dot_general(weight, pairs, contract, precision=highest)
    score_part = lax.dot_general(residual, design, contract, precision=highest)
    gram_share, score_share = (
        lax.psum_scatter(gram_part, "cell", scatter_dimension=0, tiled=True),
        lax.psum_scatter(score_part, "cell", scatter_dimension=0, tiled=True),
    )
    step_share = newton_solve(gram_share, score_share)
    beta_step = lax.all_gather(step_share, "cell", axis=0, tiled=True)
    expected_next = jnp.exp(linear_pred + jnp.dot(beta_step, design, precision=highest))
    weight_next = expected_next * live_mask
    residual_next = (observed - expected_next) * live_mask
    factors_wide = factors.astype(jnp.float32)
    loads_wide = loadings.astype(jnp.float32)
    grad_load = jnp.dot(residual_next, factors_wide, precision=highest)
    curv_load = jnp.dot(weight_next, factors_wide * factors_wide, precision=highest)
    back = (((0,), (0,)), ((), ()))
    grad_fact = lax.dot_general(residual_next, loads_wide, back, precision=highest)
    curv_fact = lax.dot_general(weight_next, loads_wide * loads_wide, back, precision=highest)
    grad_load, curv_load = lax.psum((grad_load, curv_load), "cell")
    grad_fact, curv_fact = lax.psum((grad_fact, curv_fact), "gene")
    factor_step = grad_fact / (curv_fact + 1.0)
    loading_score = grad_load / jnp.sqrt(curv_load + 1.0)
    return (beta_step, factor_step, loading_score)


MESH = pl.DeviceIdType.MESH
F32, BF16 = jnp.float32, jnp.bfloat16
VM = pl.BlockSpec(memory_space=pltpu.VMEM)
ROWS_BY_ROWS = (((1,), (1,)), ((), ()))
ACROSS = (((1,), (0,)), ((), ()))
DOWN = (((0,), (0,)), ((), ()))
LIMIT = 40 * 1024 * 1024


def split(x):
    high = x.astype(BF16)
    return high, (x - high.astype(F32)).astype(BF16)


def mul(a, b, dims):
    return lax.dot_general(a, b, dims, preferred_element_type=F32)


def remote(src, dst, send, recv, where):
    return pltpu.make_async_remote_copy(
        src_ref=src, dst_ref=dst, send_sem=send, recv_sem=recv, device_id=where, device_id_type=MESH
    )


def meet_signal(groups):
    barrier = pltpu.get_barrier_semaphore()
    count = 0
    for axis, n in groups:
        me = lax.axis_index(axis)
        for d in range(1, n):
            pl.semaphore_signal(
                barrier, inc=1, device_id={axis: lax.rem(me + d, n)}, device_id_type=MESH
            )
        count += n - 1
    return lambda: pl.semaphore_wait(barrier, count)


def design_of(knot_ref, frac_ref, cov_ref):
    slots = knot_ref.shape[1]
    levels = lax.broadcasted_iota(jnp.int32, (SPL, slots), 0)
    knot, frac = knot_ref[...], frac_ref[...]
    hats = jnp.where(levels == knot, 1.0 - frac, 0.0)
    hats = hats + jnp.where(levels == knot + 1, frac, 0.0)
    return hats, cov_ref[...]


def build_pairs(hats, cov, pair_hi, pair_lo):
    slots = hats.shape[1]
    ncov = cov.shape[0]
    half = ncov // 2

    def put(at, block):
        high, low = split(block)
        pair_hi[at : at + block.shape[0]] = high
        pair_lo[at : at + block.shape[0]] = low

    at = 0
    for p in range(SPL):
        put(at, hats[p : p + 1] * cov)
        at += ncov
    for i in range(half):
        put(at, cov[i : i + 1] * cov)
        at += ncov
    for i in range(half, ncov, 2):
        put(
            at,
            jnp.concatenate(
                [cov[i : i + 1] * cov[half:], cov[i + 1 : i + 2] * cov[half:]], axis=0
            ),
        )
        at += ncov
    put(at, hats * hats)
    at += SPL
    later = jnp.concatenate([hats[1:], jnp.zeros((1, slots), F32)], axis=0)
    put(at, hats * later)
    at += SPL
    put(at, jnp.zeros((SPL + ncov, slots), F32))


def solve(g, x):
    half = SPL // 2
    cov_at, low_at, hat_at = SPL * SPL, SPL * SPL + half * SPL, SPL * SPL + half * SPL + half * half
    off_at, score_at = hat_at + SPL, hat_at + 2 * SPL
    spot = lax.broadcasted_iota(jnp.int32, (half, g.shape[1]), 0)

    def one(block, i):
        return block[i : i + 1]

    lo = {}
    hi = {}
    for i in range(SPL):
        unit = jnp.where(spot == i % half, ridge_weight, 0.0)
        if i < half:
            lo[i] = g[cov_at + i * SPL : cov_at + i * SPL + half] + unit
            hi[i] = g[cov_at + i * SPL + half : cov_at + (i + 1) * SPL]
        else:
            hi[i] = g[low_at + (i - half) * half : low_at + (i - half + 1) * half] + unit
    b_lo = g[score_at + SPL : score_at + SPL + half]
    b_hi = g[score_at + SPL + half : score_at + 2 * SPL]
    sums_lo, sums_hi = g[0:half], g[half:SPL]
    for p in range(1, SPL):
        sums_lo = sums_lo + g[p * SPL : p * SPL + half]
        sums_hi = sums_hi + g[p * SPL + half : (p + 1) * SPL]
    b_lo, b_hi = b_lo - sums_lo, b_hi - sums_hi
    pivot_inv, edge, side_lo, side_hi, rest = [], [], [], [], []
    for p in range(SPL):
        own = g[hat_at + p : hat_at + p + 1]
        after = g[off_at + p : off_at + p + 1]
        d = own + ridge_weight
        u_lo = g[p * SPL : p * SPL + half]
        u_hi = g[p * SPL + half : (p + 1) * SPL]
        b = g[score_at + p : score_at + p + 1] - own - after
        if p > 0:
            b = b - edge[-1]
            ratio = edge[-1] * pivot_inv[-1]
            d = d - ratio * edge[-1]
            u_lo = u_lo - ratio * side_lo[-1]
            u_hi = u_hi - ratio * side_hi[-1]
            b = b - ratio * rest[-1]
        inv = 1.0 / d
        pivot_inv.append(inv)
        edge.append(after)
        side_lo.append(u_lo)
        side_hi.append(u_hi)
        rest.append(b)
        scaled_lo, scaled_hi = u_lo * inv, u_hi * inv
        b_lo = b_lo - scaled_lo * b
        b_hi = b_hi - scaled_hi * b
        for i in range(SPL):
            if i < half:
                f = one(scaled_lo, i)
                lo[i] = lo[i] - f * u_lo
            else:
                f = one(scaled_hi, i - half)
            hi[i] = hi[i] - f * u_hi
    c_inv, c_rest = [], []
    for j in range(SPL):
        if j < half:
            inv = 1.0 / one(lo[j], j)
            b = one(b_lo, j)
            s_lo = lo[j] * inv
            b_lo = b_lo - s_lo * b
        else:
            inv = 1.0 / one(hi[j], j - half)
            b = one(b_hi, j - half)
        s_hi = hi[j] * inv
        b_hi = b_hi - s_hi * b
        c_inv.append(inv)
        c_rest.append(b)
        for i in range(j + 1, SPL):
            if i < half:
                f = one(s_lo, i)
                lo[i] = lo[i] - f * lo[j]
            else:
                f = one(s_hi, i - half)
            hi[i] = hi[i] - f * hi[j]
    for j in reversed(range(SPL)):
        found = c_rest[j] * c_inv[j]
        x[SPL + j : SPL + j + 1] = found
        for i in range(j):
            c_rest[i] = c_rest[i] - (one(hi[i], j - half) if j >= half else one(lo[i], j)) * found
    x_lo, x_hi = x[SPL : SPL + half], x[SPL + half : 2 * SPL]
    after = None
    for p in reversed(range(SPL)):
        gone = jnp.sum(side_lo[p] * x_lo + side_hi[p] * x_hi, axis=0, keepdims=True)
        b = rest[p] - gone
        if after is not None:
            b = b - edge[p] * after
        after = b * pivot_inv[p]
        x[p : p + 1] = after


def pack(block, full):
    height, lanes = block.shape
    kept = height * full // lanes
    rest, part = block[kept:], lanes - full
    found = [
        pltpu.roll(rest, lanes - part - part * k, 1)[:, full:] for k in range(full // part)
    ]
    return jnp.concatenate([block[:kept, :full], jnp.concatenate(found, axis=0)], axis=1)


def unpack(target, o, full, ref):
    kept, lanes = ref.shape
    part = lanes - full
    more = kept * part // full
    target[:kept, o * full : (o + 1) * full] = ref[:, :full]
    for k in range(full // part):
        at = o * full + k * part
        target[kept:, at : at + part] = ref[k * more : (k + 1) * more, full:]


def all_kernel(
    n, m, counts_hbm, batch_hbm, live_ref, knot_hbm, frac_hbm, cov_hbm, coef_hbm, shift_hbm,
    factors_hbm, loads_hbm, beta_ref, fs_ref, ls_ref,
    batch_ref, knot_ref, frac_ref, cov_ref, factors_ref, loads_ref, p_own, p_all,
    counts, lin, rhs, pair_hi, pair_lo, tally, f_all, l_all, extra, tot_out, tot_in, known_c, known_f,
    cl_in, cl_relay, cl_out, cl_own, cl_all, w_hi, w_lo, lhs_ref, g, g_pair, g_out, g_side, g_far, tall, turned, mine,
    packed, b_all, b_cat, gl, l_pair, l_out, l_far, my_l, their_l, gf,
    c_sem, i_sem, t_send, t_recv, pz_send, pz_recv, px_send, px_recv, pp_send, pp_recv,
    gp_send, gp_recv, gs_send, gs_recv, gf_send, gf_recv, ci_send, ci_recv, ca_send, ca_recv,
    b_send, b_recv, bz_send, bz_recv, bx_send, bx_recv, bp_send, bp_recv,
    lp_send, lp_recv, lf_send, lf_recv, ol_send, ol_recv,
):
    cell, gene = lax.axis_index("cell"), lax.axis_index("gene")
    core, chip = lax.rem(cell, 2), cell // 2
    chips = n // 2
    genes, slots = counts.shape
    block = genes // chips
    rows = genes // n
    latent = loads_ref.shape[0]
    span = slots // m
    width = SPL + cov_hbm.shape[0]
    tall_p = p_own.shape[0]
    coef_ref, shift_ref = p_own.at[0:width], p_own.at[width : width + BATCHES]
    arrive = meet_signal((("cell", n), ("gene", m)))
    loads_in = []
    for i in range(n):
        at = pl.ds(i * rows, rows)
        loads_in.append(pltpu.make_async_copy(counts_hbm.at[at], counts.at[at], c_sem.at[i]))
        loads_in[-1].start()
    small = []
    for i, (source, target) in enumerate(
        (
            (batch_hbm, batch_ref), (knot_hbm, knot_ref), (frac_hbm, frac_ref), (cov_hbm, cov_ref),
            (coef_hbm, coef_ref), (shift_hbm, shift_ref), (factors_hbm, factors_ref),
            (loads_hbm, loads_ref),
        )
    ):
        small.append(pltpu.make_async_copy(source, target, i_sem.at[i]))
        small[-1].start()
    part = None
    for i in range(n):
        loads_in[i].wait()
        piece = jnp.sum(counts[i * rows : (i + 1) * rows].reshape(rows // 8, 8, slots), axis=0)
        part = piece if part is None else part + piece
    tot_out[...] = jnp.sum(part, axis=0, keepdims=True).astype(F32)
    for copy in small:
        copy.wait()
    p_own[width + BATCHES :] = loads_ref[...].astype(F32)
    arrive()
    tot = []
    for d in range(1, m):
        tot.append(
            remote(
                tot_out, tot_in.at[d - 1], t_send.at[d - 1], t_recv.at[d - 1],
                {"gene": lax.rem(gene + d, m)},
            )
        )
        tot[-1].start()

    near = gene + 1 - 2 * lax.rem(gene, 2)
    others = [near, m - 1 - gene, lax.rem(gene + 2, m)]
    beside, above = chip + 1 - 2 * lax.rem(chip, 2), lax.rem(chip + 2, chips)
    places = [chips - 1 - chip, beside, above, chip]
    partner = cell + 1 - 2 * core
    deep, broad = tall_p // 2, genes // 2
    p_cols = pl.ds(pl.multiple_of(core * broad, broad), broad)
    p_rows = [
        pl.ds(0, tall_p),
        pl.ds(pl.multiple_of(lax.rem(chip, 2) * deep, deep), deep),
        pl.ds(pl.multiple_of(chip // 2 * deep, deep), deep),
    ]
    p_line = {}
    for i in (1, 2, 0):
        p_line[i] = remote(
            p_own.at[p_rows[i], p_cols], p_all.at[gene, p_rows[i], p_cols], pz_send.at[i],
            pz_recv.at[i], {"gene": others[i]},
        )
    p_line[0].start()
    p_plane = {}

    def p_forward(i, place):
        p_line[i].wait()
        piece = p_all.at[others[i], p_rows[i], p_cols]
        p_plane[i] = remote(
            piece, piece, px_send.at[i - 1], px_recv.at[i - 1], {"cell": 2 * place + core}
        )
        p_plane[i].start()

    hats, cov = design_of(knot_ref, frac_ref, cov_ref)
    design_hi, design_lo = split(jnp.concatenate([hats, cov], axis=0))
    hot = lax.broadcasted_iota(jnp.int32, (BATCHES, slots), 0) == batch_ref[...]
    hot = jnp.where(hot, 1.0, 0.0).astype(BF16)
    rhs[0:width] = design_hi
    rhs[width : 2 * width] = design_hi
    rhs[2 * width : 3 * width] = design_lo
    rhs[3 * width : 3 * width + BATCHES] = hot
    rhs[3 * width + BATCHES : 3 * width + 2 * BATCHES] = hot
    rhs[3 * width + 2 * BATCHES :] = factors_ref[...]
    coef_hi, coef_lo = split(coef_ref[...])
    shift_hi, shift_lo = split(shift_ref[...])
    lhs = jnp.concatenate([coef_hi, coef_lo, coef_hi, shift_hi, shift_lo, loads_ref[...]], axis=0)
    lin[...] = mul(lhs, rhs[...], DOWN)
    build_pairs(hats, cov, pair_hi, pair_lo)
    live = lax.broadcasted_iota(jnp.int32, (1, slots), 1) < live_ref[0]
    mask = jnp.where(live, 1.0, 0.0)
    mask_bf = mask.astype(BF16)
    factors_live = factors_ref[...].astype(F32) * mask
    tally[0:width] = design_hi * mask_bf
    tally[width : 2 * width] = design_lo * mask_bf
    tally[2 * width :] = factors_live.astype(BF16)
    known_c[...] = mul(counts[...].astype(F32).astype(BF16), tally[...], ROWS_BY_ROWS)

    total = tot_out[...]
    for d in range(1, m):
        tot[d - 1].wait()
        total = total + tot_in[d - 1]
    extra[0:1] = jnp.where(live, jnp.log((1.0 + total) / GENES), -1e30)
    for i in (1, 2):
        p_line[i].start()

    wide = g.shape[3]
    cut = rows // 2
    upper, lower = slice(0, cut), slice(cut, rows)

    def gram_chunk(j):
        at = pl.ds(pl.multiple_of(places[j] * block, block), block)
        linear = lin[at] + extra[0:1]
        lin[at] = linear
        high, low = split(jnp.exp(linear))
        both = mul(jnp.concatenate([high, low], axis=0), pair_hi[...], ROWS_BY_ROWS)
        gram = both[:block] + both[block:] + mul(high, pair_lo[...], ROWS_BY_ROWS)
        counted = known_c[at, 0:width] + known_c[at, width : 2 * width]
        g[j, :, :, : wide - width] = gram[:, : wide - width].reshape(2, rows, wide - width)
        g[j, :, :, wide - width :] = counted.reshape(2, rows, width)
        copy = remote(
            g.at[j, 1 - core], g_pair.at[j], gp_send.at[j], gp_recv.at[j], {"cell": partner}
        )
        copy.start()
        return copy

    def onward(j, part, target, send, recv, place):
        copy = remote(g_out.at[j, part], target, send, recv, {"cell": 2 * place + core})
        copy.start()
        return copy

    pair = [gram_chunk(0), gram_chunk(1)]
    pair[0].wait()
    g_out[0] = g[0, core] + g_pair[0]
    side = [
        onward(0, upper, g_side.at[0], gs_send.at[0], gs_recv.at[0], beside),
        onward(0, lower, g_side.at[1], gs_send.at[1], gs_recv.at[1], above),
    ]
    pair.append(gram_chunk(2))
    pair[1].wait()
    g_out[1, upper] = g[1, core, upper] + g_pair[1, upper]
    far = [onward(1, upper, g_far.at[0, upper], gf_send.at[0], gf_recv.at[0], beside)]
    pair.append(gram_chunk(3))
    pair[2].wait()
    g_out[2, lower] = g[2, core, lower] + g_pair[2, lower]
    far.append(onward(2, lower, g_far.at[1, lower], gf_send.at[1], gf_recv.at[1], above))

    f_hi, f_lo = split(factors_live * factors_live)
    f_all[0:latent] = tally[2 * width :]
    f_all[latent : 2 * latent] = f_hi
    f_all[2 * latent :] = f_lo
    loads_wide = loads_ref[...].astype(F32)
    l_hi, l_lo = split(loads_wide * loads_wide)
    l_all[0:latent] = loads_ref[...]
    l_all[latent : 2 * latent] = l_hi
    l_all[2 * latent :] = l_lo

    known_f[...] = mul(l_all[0:latent], counts[...].astype(F32).astype(BF16), ACROSS) * mask

    def span_of(z):
        return pl.ds(pl.multiple_of(z * span, span), span)

    row = gene // 2
    middle = lax.rem(gene + row, 2)
    far_mid, far_end = 2 - row, 3 - 3 * row

    def cl_copy(source, target, k, slot, place):
        return remote(source, target, ci_send.at[k], ci_recv.at[slot], {"gene": place})

    cl_ahead = [
        cl_copy(known_f.at[:, span_of(z)], cl_relay.at[k], k, 2 + k, near)
        for k, z in enumerate((far_mid, far_end))
    ]
    cl_joined = [
        cl_copy(cl_out.at[k], cl_in.at[1], k, 1, z) for k, z in enumerate((far_mid, far_end))
    ]
    cl_close = cl_copy(known_f.at[:, span_of(near)], cl_in.at[0], 2, 0, near)

    @pl.when(middle == 0)
    def _():
        cl_ahead[0].start()
        cl_ahead[1].start()

    cl_close.start()

    side[1].wait()
    g_out[1, lower] = g[1, core, lower] + g_pair[1, lower] + g_side[1]
    far.append(onward(1, lower, g_far.at[0, lower], gf_send.at[2], gf_recv.at[2], beside))
    side[0].wait()
    g_out[2, upper] = g[2, core, upper] + g_pair[2, upper] + g_side[0]
    far.append(onward(2, upper, g_far.at[1, upper], gf_send.at[3], gf_recv.at[3], above))
    pair[3].wait()
    total = g[3, core] + g_pair[3]

    @pl.when(middle == 1)
    def _():
        for k, z in enumerate((far_mid, far_end)):
            cl_ahead[k].wait_recv()
            cl_out[k] = known_f[:, span_of(z)] + cl_relay[k]
            cl_joined[k].start()

    for copy in far:
        copy.wait()
    total = total + g_far[0] + g_far[1]
    tall[0:rows] = total
    if rows < 128:
        tall[rows:128] = jnp.zeros((128 - rows, wide), F32)
    turned[...] = tall[...].T
    solve(turned, mine)
    packed[...] = pack(mine[...], rows)
    b_line = []
    for i, z in enumerate(others):
        b_line.append(
            remote(packed, b_all.at[gene, core, chip], bz_send.at[i], bz_recv.at[i], {"gene": z})
        )
        b_line[-1].start()
    out = []
    for d in range(1, n):
        out.append(
            remote(
                packed, b_all.at[gene, core, chip], b_send.at[d - 1], b_recv.at[d - 1],
                {"cell": lax.rem(cell + d, n)},
            )
        )
        out[-1].start()
    b_all[gene, core, chip] = packed[...]

    b_plane = {}

    def b_forward(i):
        b_line[i].wait()
        piece = b_all.at[others[i], core, chip]
        for k in range(chips - 1):
            b_plane[i, k] = remote(
                piece, piece, bx_send.at[i, k], bx_recv.at[i, k], {"cell": 2 * places[k] + core}
            )
            b_plane[i, k].start()

    b_pair = []

    def b_swap(i):
        for k in range(chips - 1):
            b_plane[i, k].wait()
        half = b_all.at[others[i], core]
        b_pair.append(remote(half, half, bp_send.at[i], bp_recv.at[i], {"cell": partner}))
        b_pair[-1].start()

    b_forward(0)
    p_pair = []

    def p_swap(i):
        half = p_all.at[others[i], :, p_cols]
        p_pair.append(remote(half, half, pp_send.at[i], pp_recv.at[i], {"cell": partner}))
        p_pair[-1].start()

    p_line[0].wait()
    p_swap(0)
    p_forward(1, beside)
    p_forward(2, above)
    for copy in out:
        copy.wait()

    def gather_betas(z):
        for o in range(n):
            unpack(b_cat, o, rows, b_all.at[z, o % 2, o // 2])
        return b_cat[...]

    beta = gather_betas(gene)
    beta_ref[...] = beta
    beta_hi, beta_lo = split(beta)
    lhs_ref[...] = jnp.concatenate([beta_hi, beta_lo, beta_hi], axis=0).astype(F32).T.astype(BF16)
    b_forward(1)
    b_forward(2)

    lpair, lfar = [], []

    def hand_on(j):
        lpair[j].wait()
        l_out[j] = gl[j, core] + l_pair[j]
        lfar.append(
            remote(
                l_out.at[j], l_far.at[j], lf_send.at[j], lf_recv.at[j],
                {"cell": 2 * places[j] + core},
            )
        )
        lfar[-1].start()

    for j in range(chips):
        at = pl.ds(pl.multiple_of(places[j] * block, block), block)
        delta = mul(lhs_ref[at], rhs[0 : 3 * width], ACROSS)
        high, low = split(jnp.exp(lin[at] + delta))
        w_hi[at] = high
        w_lo[at] = low
        first = mul(high, f_all[...], ROWS_BY_ROWS)
        second = mul(low, f_all[0 : 2 * latent], ROWS_BY_ROWS)
        grad = known_c[at, 2 * width :] - first[:, :latent] - second[:, :latent]
        curv = first[:, latent : 2 * latent] + first[:, 2 * latent :] + second[:, latent:]
        gl[j] = jnp.concatenate([grad, curv], axis=1).reshape(2, rows, 2 * latent)
        lpair.append(
            remote(gl.at[j, 1 - core], l_pair.at[j], lp_send.at[j], lp_recv.at[j], {"cell": partner})
        )
        lpair[-1].start()
        if j > 0:
            hand_on(j - 1)
        if j == 1:
            b_swap(0)

    def gene_sums(loads, high, low):
        first = mul(loads, high, ACROSS)
        second = mul(loads[0 : 2 * latent], low, ACROSS)
        grad = first[:latent] + second[:latent]
        curv = first[latent : 2 * latent] + first[2 * latent :] + second[latent:]
        return jnp.concatenate([grad, curv], axis=0)

    for i in (1, 2):
        p_plane[i].wait()
        p_swap(i)
    gf[...] = gene_sums(l_all[...], w_hi[...], w_lo[...])

    def other_genes(i):
        z = others[i]
        p_pair[i].wait()
        b_pair[i].wait()
        next_hi, next_lo = split(p_all[z, 0:width] + gather_betas(z))
        shift_hi, shift_lo = split(p_all[z, width : width + BATCHES])
        wider = p_all[z, width + BATCHES :]
        one = wider.astype(BF16)
        two_hi, two_lo = split(wider * wider)
        lhs = jnp.concatenate([next_hi, next_lo, next_hi, shift_hi, shift_lo, one], axis=0)
        high, low = split(jnp.exp(mul(lhs, rhs[...], DOWN) + extra[0:1]))
        gf[...] += gene_sums(jnp.concatenate([one, two_hi, two_lo], axis=0), high, low)

    cl_close.wait()
    cl_joined[0].wait_recv()
    cl_joined[0].wait_send()
    cl_joined[1].wait_send()
    cl_own[...] = known_f[:, span_of(gene)] + cl_in[0] + cl_in[1]
    ca_line = []
    for i, z in enumerate(others):
        ca_line.append(
            remote(cl_own, cl_all.at[gene], ca_send.at[i], ca_recv.at[gene], {"gene": z})
        )
        ca_line[-1].start()
    cl_all[gene] = cl_own[...]

    lpair[-1].wait()
    total = gl[chips - 1, core] + l_pair[chips - 1]
    b_swap(1)
    b_swap(2)
    other_genes(0)
    for j in range(chips - 1):
        lfar[j].wait()
        total = total + l_far[j]
    if rows < 128:
        total = jnp.concatenate([total, jnp.zeros((128 - rows, 2 * latent), F32)], axis=0)
    total = total.T
    my_l[...] = pack(total[:latent] / jnp.sqrt(total[latent:] + 1.0), rows)
    out_l = []
    for d in range(1, n):
        out_l.append(
            remote(
                my_l, their_l.at[cell], ol_send.at[d - 1], ol_recv.at[d - 1],
                {"cell": lax.rem(cell + d, n)},
            )
        )
        out_l[-1].start()
    their_l[cell] = my_l[...]
    other_genes(1)
    other_genes(2)
    for z in others:
        remote(cl_own, cl_all.at[z], ca_send.at[0], ca_recv.at[z], {"gene": near}).wait_recv()
    for o in range(m):
        at = slice(o * span, (o + 1) * span)
        fs_ref[:, at] = (cl_all[o] - gf[:latent, at]) / (gf[latent:, at] + 1.0)
    for d in range(1, n):
        out_l[d - 1].wait()
    for o in range(n):
        unpack(ls_ref, o, rows, their_l.at[o])
    for copy in ca_line:
        copy.wait_send()


def pass_on(*refs):
    count = len(refs) // 2
    for source, target in zip(refs[:count], refs[count:]):
        target[...] = source[...]


def local_fused(
    n, m, counts, batch_id, live_cells, knot_bin, depth_frac, cell_covariates, coefficients,
    batch_effect, factors, loadings,
):
    genes, slots = counts.shape
    rows, span, latent = genes // n, slots // m, factors.shape[1]
    ncov = cell_covariates.shape[0]
    width = SPL + ncov
    wide = SPL * ncov + ncov * ncov * 3 // 4 + 2 * SPL + width
    chips = n // 2
    dma = pltpu.SemaphoreType.DMA
    shape = jax.ShapeDtypeStruct
    vmem = pltpu.VMEM

    def params(**kw):
        return pltpu.CompilerParams(vmem_limit_bytes=LIMIT, **kw)

    def stay(x):
        return pltpu.with_memory_space_constraint(x, pltpu.HBM)

    knot, frac, batch = (v.reshape(1, slots) for v in (knot_bin, depth_frac, batch_id))
    shapes = (shape((width, genes), F32), shape((latent, slots), F32), shape((latent, genes), F32))
    there = pl.BlockSpec(memory_space=pl.ANY)
    found = pl.pallas_call(
        functools.partial(all_kernel, n, m),
        out_shape=shapes,
        in_specs=[there, there, pl.BlockSpec(memory_space=pltpu.SMEM)] + [there] * 7,
        out_specs=(VM, VM, VM),
        scratch_shapes=[
            vmem((1, slots), jnp.int32),
            vmem((1, slots), jnp.int32),
            vmem((1, slots), F32),
            vmem((ncov, slots), F32),
            vmem((latent, slots), BF16),
            vmem((latent, genes), BF16),
            vmem((width + BATCHES + latent, genes), F32),
            vmem((m, width + BATCHES + latent, genes), F32),
            vmem((genes, slots), jnp.int32),
            vmem((genes, slots), F32),
            vmem((3 * width + 2 * BATCHES + latent, slots), BF16),
            vmem((wide, slots), BF16),
            vmem((wide, slots), BF16),
            vmem((2 * width + latent, slots), BF16),
            vmem((3 * latent, slots), BF16),
            vmem((3 * latent, genes), BF16),
            vmem((8, slots), F32),
            vmem((1, slots), F32),
            vmem((m - 1, 1, slots), F32),
            vmem((genes, 2 * width + latent), F32),
            vmem((latent, slots), F32),
            vmem((2, latent, span), F32),
            vmem((2, latent, span), F32),
            vmem((2, latent, span), F32),
            vmem((latent, span), F32),
            vmem((m, latent, span), F32),
            vmem((genes, slots), BF16),
            vmem((genes, slots), BF16),
            vmem((genes, 3 * width), BF16),
            vmem((chips, 2, rows, wide), F32),
            vmem((chips, rows, wide), F32),
            vmem((chips - 1, rows, wide), F32),
            vmem((2, rows // 2, wide), F32),
            vmem((2, rows, wide), F32),
            vmem((128, wide), F32),
            vmem((wide, 128), F32),
            vmem((width, 128), F32),
            vmem((width * rows // 128, 128), F32),
            vmem((m, 2, chips, width * rows // 128, 128), F32),
            vmem((width, genes), F32),
            vmem((chips, 2, rows, 2 * latent), F32),
            vmem((chips, rows, 2 * latent), F32),
            vmem((chips - 1, rows, 2 * latent), F32),
            vmem((chips - 1, rows, 2 * latent), F32),
            vmem((latent * rows // 128, 128), F32),
            vmem((n, latent * rows // 128, 128), F32),
            vmem((2 * latent, slots), F32),
            dma((n,)), dma((8,)), dma((m - 1,)), dma((m - 1,)),
            dma((m - 1,)), dma((m - 1,)), dma((2,)), dma((2,)),
            dma((m - 1,)), dma((m - 1,)),
            dma((chips,)), dma((chips,)), dma((2,)), dma((2,)), dma((4,)), dma((4,)),
            dma((m - 1,)), dma((m,)), dma((m - 1,)), dma((m,)),
            dma((n - 1,)), dma((n - 1,)), dma((m - 1,)), dma((m - 1,)),
            dma((m - 1, chips - 1)), dma((m - 1, chips - 1)), dma((m - 1,)), dma((m - 1,)),
            dma((chips,)), dma((chips,)), dma((chips - 1,)), dma((chips - 1,)),
            dma((n - 1,)), dma((n - 1,)),
        ],
        compiler_params=params(collective_id=0, has_side_effects=True),
        name="step",
    )(
        stay(counts), stay(batch), live_cells, stay(knot), stay(frac), stay(cell_covariates),
        stay(coefficients.T), stay(batch_effect.T), stay(factors.T), stay(loadings.T),
    )
    beta, fs, ls = pl.pallas_call(
        pass_on, out_shape=shapes, in_specs=[VM] * 3, out_specs=(VM, VM, VM),
        compiler_params=params(), name="finish",
    )(*found)
    return beta.T, fs.T, ls.T


def local(n, m, *args):
    counts, cov, factors = args[0], args[5], args[8]
    genes, slots = counts.shape
    fits = (
        n == 8
        and m == 4
        and genes % (16 * n) == 0
        and genes // n == 96
        and slots % (128 * m) == 0
        and genes % 256 == 0
        and (SPL + cov.shape[0] + BATCHES + factors.shape[1]) % 16 == 0
        and cov.shape[0] == SPL
        and factors.shape[1] == 64
    )
    if fits:
        return local_fused(n, m, *args)
    return local_plain(*args)


def solution(mesh):
    placed = (
        P("gene", "cell"),
        P("cell"),
        P("cell"),
        P("cell"),
        P("cell"),
        P(None, "cell"),
        P("gene", None),
        P("gene", None),
        P("cell", None),
        P("gene", None),
    )
    return jax.shard_map(
        functools.partial(local, mesh.shape["cell"], mesh.shape["gene"]),
        mesh=mesh,
        in_specs=placed,
        out_specs=(P("gene", None), P("cell", None), P("gene", None)),
        check_vma=False,
    )
```

```python
import functools

import jax
import jax.numpy as jnp
from jax import lax
from jax.experimental import pallas as pl
from jax.experimental.pallas import tpu as pltpu
from jax.sharding import PartitionSpec as P

GENES = 3072
SPL = 16
BATCHES = 64


ridge_weight = 1.0


def design_rows(knot_bin, depth_frac, cell_covariates):
    levels = jnp.arange(SPL, dtype=jnp.int32)[:, None]
    fraction = depth_frac[None, :]
    hat_basis = jnp.where(levels == knot_bin[None, :], 1.0 - fraction, 0.0)
    hat_basis = hat_basis + jnp.where(levels == knot_bin[None, :] + 1, fraction, 0.0)
    return jnp.concatenate([hat_basis, cell_covariates], axis=0)


def newton_solve(gram_flat, score):
    columns = score.shape[-1]
    identity = jnp.eye(columns, dtype=gram_flat.dtype)
    system = gram_flat.reshape(-1, columns, columns) + ridge_weight * identity
    factor_lower = jnp.linalg.cholesky(system)
    middle = jax.scipy.linalg.solve_triangular(factor_lower, score[..., None], lower=True)
    return jax.scipy.linalg.solve_triangular(factor_lower, middle, lower=True, trans=1)[..., 0]


def local_plain(
    counts,
    batch_id,
    live_cells,
    knot_bin,
    depth_frac,
    cell_covariates,
    coefficients,
    batch_effect,
    factors,
    loadings,
):
    highest = lax.Precision.HIGHEST
    contract = (((1,), (1,)), ((), ()))
    observed = counts.astype(jnp.float32)
    totals = lax.psum(jnp.sum(observed, axis=0), "gene")
    offset = jnp.log((1.0 + totals) / GENES)
    slot_count = observed.shape[1]
    live_mask = (jnp.arange(slot_count, dtype=jnp.int32) < live_cells[0]).astype(jnp.float32)
    design = design_rows(knot_bin, depth_frac, cell_covariates)
    columns = design.shape[0]
    onehot = (jnp.arange(BATCHES, dtype=jnp.int32)[:, None] == batch_id[None, :]).astype(
        jnp.float32
    )
    stacked = jnp.concatenate([design, onehot], axis=0)
    linear = jnp.dot(
        jnp.concatenate([coefficients, batch_effect], axis=1), stacked, precision=highest
    )
    latent = lax.dot_general(loadings, factors, contract, preferred_element_type=jnp.float32)
    linear_pred = offset[None, :] + linear + latent
    expected = jnp.exp(linear_pred)
    weight = expected * live_mask
    residual = (observed - expected) * live_mask
    pairs = (design[:, None, :] * design[None, :, :]).reshape(columns * columns, slot_count)
    gram_part = lax.dot_general(weight, pairs, contract, precision=highest)
    score_part = lax.dot_general(residual, design, contract, precision=highest)
    gram_share, score_share = (
        lax.psum_scatter(gram_part, "cell", scatter_dimension=0, tiled=True),
        lax.psum_scatter(score_part, "cell", scatter_dimension=0, tiled=True),
    )
    step_share = newton_solve(gram_share, score_share)
    beta_step = lax.all_gather(step_share, "cell", axis=0, tiled=True)
    expected_next = jnp.exp(linear_pred + jnp.dot(beta_step, design, precision=highest))
    weight_next = expected_next * live_mask
    residual_next = (observed - expected_next) * live_mask
    factors_wide = factors.astype(jnp.float32)
    loads_wide = loadings.astype(jnp.float32)
    grad_load = jnp.dot(residual_next, factors_wide, precision=highest)
    curv_load = jnp.dot(weight_next, factors_wide * factors_wide, precision=highest)
    back = (((0,), (0,)), ((), ()))
    grad_fact = lax.dot_general(residual_next, loads_wide, back, precision=highest)
    curv_fact = lax.dot_general(weight_next, loads_wide * loads_wide, back, precision=highest)
    grad_load, curv_load = lax.psum((grad_load, curv_load), "cell")
    grad_fact, curv_fact = lax.psum((grad_fact, curv_fact), "gene")
    factor_step = grad_fact / (curv_fact + 1.0)
    loading_score = grad_load / jnp.sqrt(curv_load + 1.0)
    return (beta_step, factor_step, loading_score)


MESH = pl.DeviceIdType.MESH
F32, BF16 = jnp.float32, jnp.bfloat16
VM = pl.BlockSpec(memory_space=pltpu.VMEM)
ROWS_BY_ROWS = (((1,), (1,)), ((), ()))
ACROSS = (((1,), (0,)), ((), ()))
DOWN = (((0,), (0,)), ((), ()))
LIMIT = 40 * 1024 * 1024


def split(x):
    high = x.astype(BF16)
    return high, (x - high.astype(F32)).astype(BF16)


def mul(a, b, dims):
    return lax.dot_general(a, b, dims, preferred_element_type=F32)


def remote(src, dst, send, recv, where):
    return pltpu.make_async_remote_copy(
        src_ref=src, dst_ref=dst, send_sem=send, recv_sem=recv, device_id=where, device_id_type=MESH
    )


def meet_signal(groups):
    barrier = pltpu.get_barrier_semaphore()
    count = 0
    for axis, n in groups:
        me = lax.axis_index(axis)
        for d in range(1, n):
            pl.semaphore_signal(
                barrier, inc=1, device_id={axis: lax.rem(me + d, n)}, device_id_type=MESH
            )
        count += n - 1
    return lambda: pl.semaphore_wait(barrier, count)


def design_of(knot_ref, frac_ref, cov_ref):
    slots = knot_ref.shape[1]
    levels = lax.broadcasted_iota(jnp.int32, (SPL, slots), 0)
    knot, frac = knot_ref[...], frac_ref[...]
    hats = jnp.where(levels == knot, 1.0 - frac, 0.0)
    hats = hats + jnp.where(levels == knot + 1, frac, 0.0)
    return hats, cov_ref[...]


def build_pairs(hats, cov, pair_hi, pair_lo):
    slots = hats.shape[1]
    ncov = cov.shape[0]
    half = ncov // 2

    def put(at, block):
        high, low = split(block)
        pair_hi[at : at + block.shape[0]] = high
        pair_lo[at : at + block.shape[0]] = low

    at = 0
    for p in range(SPL):
        put(at, hats[p : p + 1] * cov)
        at += ncov
    for i in range(half):
        put(at, cov[i : i + 1] * cov)
        at += ncov
    for i in range(half, ncov, 2):
        put(
            at,
            jnp.concatenate(
                [cov[i : i + 1] * cov[half:], cov[i + 1 : i + 2] * cov[half:]], axis=0
            ),
        )
        at += ncov
    put(at, hats * hats)
    at += SPL
    later = jnp.concatenate([hats[1:], jnp.zeros((1, slots), F32)], axis=0)
    put(at, hats * later)
    at += SPL
    put(at, jnp.zeros((SPL + ncov, slots), F32))


def solve(g, x):
    half = SPL // 2
    cov_at, low_at, hat_at = SPL * SPL, SPL * SPL + half * SPL, SPL * SPL + half * SPL + half * half
    off_at, score_at = hat_at + SPL, hat_at + 2 * SPL
    spot = lax.broadcasted_iota(jnp.int32, (half, g.shape[1]), 0)

    def one(block, i):
        return block[i : i + 1]

    lo = {}
    hi = {}
    for i in range(SPL):
        unit = jnp.where(spot == i % half, ridge_weight, 0.0)
        if i < half:
            lo[i] = g[cov_at + i * SPL : cov_at + i * SPL + half] + unit
            hi[i] = g[cov_at + i * SPL + half : cov_at + (i + 1) * SPL]
        else:
            hi[i] = g[low_at + (i - half) * half : low_at + (i - half + 1) * half] + unit
    b_lo = g[score_at + SPL : score_at + SPL + half]
    b_hi = g[score_at + SPL + half : score_at + 2 * SPL]
    sums_lo, sums_hi = g[0:half], g[half:SPL]
    for p in range(1, SPL):
        sums_lo = sums_lo + g[p * SPL : p * SPL + half]
        sums_hi = sums_hi + g[p * SPL + half : (p + 1) * SPL]
    b_lo, b_hi = b_lo - sums_lo, b_hi - sums_hi
    pivot_inv, edge, side_lo, side_hi, rest = [], [], [], [], []
    for p in range(SPL):
        own = g[hat_at + p : hat_at + p + 1]
        after = g[off_at + p : off_at + p + 1]
        d = own + ridge_weight
        u_lo = g[p * SPL : p * SPL + half]
        u_hi = g[p * SPL + half : (p + 1) * SPL]
        b = g[score_at + p : score_at + p + 1] - own - after
        if p > 0:
            b = b - edge[-1]
            ratio = edge[-1] * pivot_inv[-1]
            d = d - ratio * edge[-1]
            u_lo = u_lo - ratio * side_lo[-1]
            u_hi = u_hi - ratio * side_hi[-1]
            b = b - ratio * rest[-1]
        inv = 1.0 / d
        pivot_inv.append(inv)
        edge.append(after)
        side_lo.append(u_lo)
        side_hi.append(u_hi)
        rest.append(b)
        scaled_lo, scaled_hi = u_lo * inv, u_hi * inv
        b_lo = b_lo - scaled_lo * b
        b_hi = b_hi - scaled_hi * b
        for i in range(SPL):
            if i < half:
                f = one(scaled_lo, i)
                lo[i] = lo[i] - f * u_lo
            else:
                f = one(scaled_hi, i - half)
            hi[i] = hi[i] - f * u_hi
    c_inv, c_rest = [], []
    for j in range(SPL):
        if j < half:
            inv = 1.0 / one(lo[j], j)
            b = one(b_lo, j)
            s_lo = lo[j] * inv
            b_lo = b_lo - s_lo * b
        else:
            inv = 1.0 / one(hi[j], j - half)
            b = one(b_hi, j - half)
        s_hi = hi[j] * inv
        b_hi = b_hi - s_hi * b
        c_inv.append(inv)
        c_rest.append(b)
        for i in range(j + 1, SPL):
            if i < half:
                f = one(s_lo, i)
                lo[i] = lo[i] - f * lo[j]
            else:
                f = one(s_hi, i - half)
            hi[i] = hi[i] - f * hi[j]
    for j in reversed(range(SPL)):
        found = c_rest[j] * c_inv[j]
        x[SPL + j : SPL + j + 1] = found
        for i in range(j):
            c_rest[i] = c_rest[i] - (one(hi[i], j - half) if j >= half else one(lo[i], j)) * found
    x_lo, x_hi = x[SPL : SPL + half], x[SPL + half : 2 * SPL]
    after = None
    for p in reversed(range(SPL)):
        gone = jnp.sum(side_lo[p] * x_lo + side_hi[p] * x_hi, axis=0, keepdims=True)
        b = rest[p] - gone
        if after is not None:
            b = b - edge[p] * after
        after = b * pivot_inv[p]
        x[p : p + 1] = after


def pack(block, full):
    height, lanes = block.shape
    kept = height * full // lanes
    rest, part = block[kept:], lanes - full
    found = [
        pltpu.roll(rest, lanes - part - part * k, 1)[:, full:] for k in range(full // part)
    ]
    return jnp.concatenate([block[:kept, :full], jnp.concatenate(found, axis=0)], axis=1)


def unpack(target, o, full, ref):
    kept, lanes = ref.shape
    part = lanes - full
    more = kept * part // full
    target[:kept, o * full : (o + 1) * full] = ref[:, :full]
    for k in range(full // part):
        at = o * full + k * part
        target[kept:, at : at + part] = ref[k * more : (k + 1) * more, full:]


def all_kernel(
    n, m, counts_hbm, batch_hbm, live_ref, knot_hbm, frac_hbm, cov_hbm, coef_hbm, shift_hbm,
    factors_hbm, loads_hbm, beta_ref, fs_ref, ls_ref,
    batch_ref, knot_ref, frac_ref, cov_ref, factors_ref, loads_ref, p_own, p_all,
    counts, lin, rhs, pair_hi, pair_lo, tally, f_all, l_all, extra, tot_out, tot_in, known_c, known_f,
    cl_in, cl_relay, cl_out, cl_own, cl_all, w_hi, w_lo, lhs_ref, g, g_pair, g_out, g_side, g_far, tall, turned, mine,
    packed, b_all, b_cat, gl, l_pair, l_out, l_far, my_l, their_l, gf,
    c_sem, i_sem, t_send, t_recv, pz_send, pz_recv, px_send, px_recv, pp_send, pp_recv,
    gp_send, gp_recv, gs_send, gs_recv, gf_send, gf_recv, ci_send, ci_recv, ca_send, ca_recv,
    b_send, b_recv, bz_send, bz_recv, bx_send, bx_recv, bp_send, bp_recv,
    lp_send, lp_recv, lf_send, lf_recv, ol_send, ol_recv,
):
    cell, gene = lax.axis_index("cell"), lax.axis_index("gene")
    core, chip = lax.rem(cell, 2), cell // 2
    chips = n // 2
    genes, slots = counts.shape
    block = genes // chips
    rows = genes // n
    latent = loads_ref.shape[0]
    span = slots // m
    width = SPL + cov_hbm.shape[0]
    tall_p = p_own.shape[0]
    coef_ref, shift_ref = p_own.at[0:width], p_own.at[width : width + BATCHES]
    arrive = meet_signal((("cell", n), ("gene", m)))
    loads_in = []
    for i in range(n):
        at = pl.ds(i * rows, rows)
        loads_in.append(pltpu.make_async_copy(counts_hbm.at[at], counts.at[at], c_sem.at[i]))
        loads_in[-1].start()
    small = []
    for i, (source, target) in enumerate(
        (
            (batch_hbm, batch_ref), (knot_hbm, knot_ref), (frac_hbm, frac_ref), (cov_hbm, cov_ref),
            (coef_hbm, coef_ref), (shift_hbm, shift_ref), (factors_hbm, factors_ref),
            (loads_hbm, loads_ref),
        )
    ):
        small.append(pltpu.make_async_copy(source, target, i_sem.at[i]))
        small[-1].start()
    part = None
    for i in range(n):
        loads_in[i].wait()
        piece = jnp.sum(counts[i * rows : (i + 1) * rows].reshape(rows // 8, 8, slots), axis=0)
        part = piece if part is None else part + piece
    tot_out[...] = jnp.sum(part, axis=0, keepdims=True).astype(F32)
    for copy in small:
        copy.wait()
    p_own[width + BATCHES :] = loads_ref[...].astype(F32)
    arrive()
    tot = []
    for d in range(1, m):
        tot.append(
            remote(
                tot_out, tot_in.at[d - 1], t_send.at[d - 1], t_recv.at[d - 1],
                {"gene": lax.rem(gene + d, m)},
            )
        )
        tot[-1].start()

    near = gene + 1 - 2 * lax.rem(gene, 2)
    others = [near, m - 1 - gene, lax.rem(gene + 2, m)]
    beside, above = chip + 1 - 2 * lax.rem(chip, 2), lax.rem(chip + 2, chips)
    places = [chips - 1 - chip, beside, above, chip]
    partner = cell + 1 - 2 * core
    deep, broad = tall_p // 2, genes // 2
    p_cols = pl.ds(pl.multiple_of(core * broad, broad), broad)
    p_rows = [
        pl.ds(0, tall_p),
        pl.ds(pl.multiple_of(lax.rem(chip, 2) * deep, deep), deep),
        pl.ds(pl.multiple_of(chip // 2 * deep, deep), deep),
    ]
    p_line = {}
    for i in (1, 2, 0):
        p_line[i] = remote(
            p_own.at[p_rows[i], p_cols], p_all.at[gene, p_rows[i], p_cols], pz_send.at[i],
            pz_recv.at[i], {"gene": others[i]},
        )
    p_line[0].start()
    p_plane = {}

    def p_forward(i, place):
        p_line[i].wait()
        piece = p_all.at[others[i], p_rows[i], p_cols]
        p_plane[i] = remote(
            piece, piece, px_send.at[i - 1], px_recv.at[i - 1], {"cell": 2 * place + core}
        )
        p_plane[i].start()

    hats, cov = design_of(knot_ref, frac_ref, cov_ref)
    design_hi, design_lo = split(jnp.concatenate([hats, cov], axis=0))
    hot = lax.broadcasted_iota(jnp.int32, (BATCHES, slots), 0) == batch_ref[...]
    hot = jnp.where(hot, 1.0, 0.0).astype(BF16)
    rhs[0:width] = design_hi
    rhs[width : 2 * width] = design_hi
    rhs[2 * width : 3 * width] = design_lo
    rhs[3 * width : 3 * width + BATCHES] = hot
    rhs[3 * width + BATCHES : 3 * width + 2 * BATCHES] = hot
    rhs[3 * width + 2 * BATCHES :] = factors_ref[...]
    coef_hi, coef_lo = split(coef_ref[...])
    shift_hi, shift_lo = split(shift_ref[...])
    lhs = jnp.concatenate([coef_hi, coef_lo, coef_hi, shift_hi, shift_lo, loads_ref[...]], axis=0)
    lin[...] = mul(lhs, rhs[...], DOWN)
    build_pairs(hats, cov, pair_hi, pair_lo)
    live = lax.broadcasted_iota(jnp.int32, (1, slots), 1) < live_ref[0]
    mask = jnp.where(live, 1.0, 0.0)
    mask_bf = mask.astype(BF16)
    factors_live = factors_ref[...].astype(F32) * mask
    tally[0:width] = design_hi * mask_bf
    tally[width : 2 * width] = design_lo * mask_bf
    tally[2 * width :] = factors_live.astype(BF16)
    known_c[...] = mul(counts[...].astype(F32).astype(BF16), tally[...], ROWS_BY_ROWS)

    total = tot_out[...]
    for d in range(1, m):
        tot[d - 1].wait()
        total = total + tot_in[d - 1]
    extra[0:1] = jnp.where(live, jnp.log((1.0 + total) / GENES), -1e30)
    for i in (1, 2):
        p_line[i].start()

    wide = g.shape[3]
    cut = rows // 2
    upper, lower = slice(0, cut), slice(cut, rows)

    def gram_chunk(j):
        at = pl.ds(pl.multiple_of(places[j] * block, block), block)
        linear = lin[at] + extra[0:1]
        lin[at] = linear
        high, low = split(jnp.exp(linear))
        both = mul(jnp.concatenate([high, low], axis=0), pair_hi[...], ROWS_BY_ROWS)
        gram = both[:block] + both[block:] + mul(high, pair_lo[...], ROWS_BY_ROWS)
        counted = known_c[at, 0:width] + known_c[at, width : 2 * width]
        g[j, :, :, : wide - width] = gram[:, : wide - width].reshape(2, rows, wide - width)
        g[j, :, :, wide - width :] = counted.reshape(2, rows, width)
        copy = remote(
            g.at[j, 1 - core], g_pair.at[j], gp_send.at[j], gp_recv.at[j], {"cell": partner}
        )
        copy.start()
        return copy

    def onward(j, part, target, send, recv, place):
        copy = remote(g_out.at[j, part], target, send, recv, {"cell": 2 * place + core})
        copy.start()
        return copy

    pair = [gram_chunk(0), gram_chunk(1)]
    pair[0].wait()
    g_out[0] = g[0, core] + g_pair[0]
    side = [
        onward(0, upper, g_side.at[0], gs_send.at[0], gs_recv.at[0], beside),
        onward(0, lower, g_side.at[1], gs_send.at[1], gs_recv.at[1], above),
    ]
    pair.append(gram_chunk(2))
    pair[1].wait()
    g_out[1, upper] = g[1, core, upper] + g_pair[1, upper]
    far = [onward(1, upper, g_far.at[0, upper], gf_send.at[0], gf_recv.at[0], beside)]
    pair.append(gram_chunk(3))
    pair[2].wait()
    g_out[2, lower] = g[2, core, lower] + g_pair[2, lower]
    far.append(onward(2, lower, g_far.at[1, lower], gf_send.at[1], gf_recv.at[1], above))

    f_hi, f_lo = split(factors_live * factors_live)
    f_all[0:latent] = tally[2 * width :]
    f_all[latent : 2 * latent] = f_hi
    f_all[2 * latent :] = f_lo
    loads_wide = loads_ref[...].astype(F32)
    l_hi, l_lo = split(loads_wide * loads_wide)
    l_all[0:latent] = loads_ref[...]
    l_all[latent : 2 * latent] = l_hi
    l_all[2 * latent :] = l_lo

    known_f[...] = mul(l_all[0:latent], counts[...].astype(F32).astype(BF16), ACROSS) * mask

    def span_of(z):
        return pl.ds(pl.multiple_of(z * span, span), span)

    row = gene // 2
    middle = lax.rem(gene + row, 2)
    far_mid, far_end = 2 - row, 3 - 3 * row

    def cl_copy(source, target, k, slot, place):
        return remote(source, target, ci_send.at[k], ci_recv.at[slot], {"gene": place})

    cl_ahead = [
        cl_copy(known_f.at[:, span_of(z)], cl_relay.at[k], k, 2 + k, near)
        for k, z in enumerate((far_mid, far_end))
    ]
    cl_joined = [
        cl_copy(cl_out.at[k], cl_in.at[1], k, 1, z) for k, z in enumerate((far_mid, far_end))
    ]
    cl_close = cl_copy(known_f.at[:, span_of(near)], cl_in.at[0], 2, 0, near)

    @pl.when(middle == 0)
    def _():
        cl_ahead[0].start()
        cl_ahead[1].start()

    cl_close.start()

    side[1].wait()
    g_out[1, lower] = g[1, core, lower] + g_pair[1, lower] + g_side[1]
    far.append(onward(1, lower, g_far.at[0, lower], gf_send.at[2], gf_recv.at[2], beside))
    side[0].wait()
    g_out[2, upper] = g[2, core, upper] + g_pair[2, upper] + g_side[0]
    far.append(onward(2, upper, g_far.at[1, upper], gf_send.at[3], gf_recv.at[3], above))
    pair[3].wait()
    total = g[3, core] + g_pair[3]

    @pl.when(middle == 1)
    def _():
        for k, z in enumerate((far_mid, far_end)):
            cl_ahead[k].wait_recv()
            cl_out[k] = known_f[:, span_of(z)] + cl_relay[k]
            cl_joined[k].start()

    for copy in far:
        copy.wait()
    total = total + g_far[0] + g_far[1]
    tall[0:rows] = total
    if rows < 128:
        tall[rows:128] = jnp.zeros((128 - rows, wide), F32)
    turned[...] = tall[...].T
    solve(turned, mine)
    packed[...] = pack(mine[...], rows)
    out = []
    for d in range(1, n):
        out.append(
            remote(
                packed, b_all.at[gene, core, chip], b_send.at[d - 1], b_recv.at[d - 1],
                {"cell": lax.rem(cell + d, n)},
            )
        )
        out[-1].start()
    b_line = []
    for i, z in enumerate(others):
        b_line.append(
            remote(packed, b_all.at[gene, core, chip], bz_send.at[i], bz_recv.at[i], {"gene": z})
        )
        b_line[-1].start()
    b_all[gene, core, chip] = packed[...]

    b_plane = {}

    def b_forward(i):
        b_line[i].wait()
        piece = b_all.at[others[i], core, chip]
        for k in range(chips - 1):
            b_plane[i, k] = remote(
                piece, piece, bx_send.at[i, k], bx_recv.at[i, k], {"cell": 2 * places[k] + core}
            )
            b_plane[i, k].start()

    b_pair = []

    def b_swap(i):
        for k in range(chips - 1):
            b_plane[i, k].wait()
        half = b_all.at[others[i], core]
        b_pair.append(remote(half, half, bp_send.at[i], bp_recv.at[i], {"cell": partner}))
        b_pair[-1].start()

    b_forward(0)
    p_pair = []

    def p_swap(i):
        half = p_all.at[others[i], :, p_cols]
        p_pair.append(remote(half, half, pp_send.at[i], pp_recv.at[i], {"cell": partner}))
        p_pair[-1].start()

    p_line[0].wait()
    p_swap(0)
    p_forward(1, beside)
    p_forward(2, above)
    for copy in out:
        copy.wait()

    def gather_betas(z):
        for o in range(n):
            unpack(b_cat, o, rows, b_all.at[z, o % 2, o // 2])
        return b_cat[...]

    beta = gather_betas(gene)
    beta_ref[...] = beta
    beta_hi, beta_lo = split(beta)
    lhs_ref[...] = jnp.concatenate([beta_hi, beta_lo, beta_hi], axis=0).astype(F32).T.astype(BF16)

    lpair, lfar = [], []

    def hand_on(j):
        lpair[j].wait()
        l_out[j] = gl[j, core] + l_pair[j]
        lfar.append(
            remote(
                l_out.at[j], l_far.at[j], lf_send.at[j], lf_recv.at[j],
                {"cell": 2 * places[j] + core},
            )
        )
        lfar[-1].start()

    for j in range(chips):
        at = pl.ds(pl.multiple_of(places[j] * block, block), block)
        delta = mul(lhs_ref[at], rhs[0 : 3 * width], ACROSS)
        high, low = split(jnp.exp(lin[at] + delta))
        w_hi[at] = high
        w_lo[at] = low
        first = mul(high, f_all[...], ROWS_BY_ROWS)
        second = mul(low, f_all[0 : 2 * latent], ROWS_BY_ROWS)
        grad = known_c[at, 2 * width :] - first[:, :latent] - second[:, :latent]
        curv = first[:, latent : 2 * latent] + first[:, 2 * latent :] + second[:, latent:]
        gl[j] = jnp.concatenate([grad, curv], axis=1).reshape(2, rows, 2 * latent)
        lpair.append(
            remote(gl.at[j, 1 - core], l_pair.at[j], lp_send.at[j], lp_recv.at[j], {"cell": partner})
        )
        lpair[-1].start()
        if j > 0:
            hand_on(j - 1)
        if j == 0:
            b_forward(1)
            b_forward(2)
        if j == 1:
            b_swap(0)

    def gene_sums(loads, high, low):
        first = mul(loads, high, ACROSS)
        second = mul(loads[0 : 2 * latent], low, ACROSS)
        grad = first[:latent] + second[:latent]
        curv = first[latent : 2 * latent] + first[2 * latent :] + second[latent:]
        return jnp.concatenate([grad, curv], axis=0)

    for i in (1, 2):
        p_plane[i].wait()
        p_swap(i)
    gf[...] = gene_sums(l_all[...], w_hi[...], w_lo[...])

    def other_genes(i):
        z = others[i]
        p_pair[i].wait()
        b_pair[i].wait()
        next_hi, next_lo = split(p_all[z, 0:width] + gather_betas(z))
        shift_hi, shift_lo = split(p_all[z, width : width + BATCHES])
        wider = p_all[z, width + BATCHES :]
        one = wider.astype(BF16)
        two_hi, two_lo = split(wider * wider)
        lhs = jnp.concatenate([next_hi, next_lo, next_hi, shift_hi, shift_lo, one], axis=0)
        high, low = split(jnp.exp(mul(lhs, rhs[...], DOWN) + extra[0:1]))
        gf[...] += gene_sums(jnp.concatenate([one, two_hi, two_lo], axis=0), high, low)

    cl_close.wait()
    cl_joined[0].wait_recv()
    cl_joined[0].wait_send()
    cl_joined[1].wait_send()
    cl_own[...] = known_f[:, span_of(gene)] + cl_in[0] + cl_in[1]
    ca_line = []
    for i, z in enumerate(others):
        ca_line.append(
            remote(cl_own, cl_all.at[gene], ca_send.at[i], ca_recv.at[gene], {"gene": z})
        )
        ca_line[-1].start()
    cl_all[gene] = cl_own[...]

    lpair[-1].wait()
    total = gl[chips - 1, core] + l_pair[chips - 1]
    b_swap(1)
    b_swap(2)
    other_genes(0)
    for j in range(chips - 1):
        lfar[j].wait()
        total = total + l_far[j]
    if rows < 128:
        total = jnp.concatenate([total, jnp.zeros((128 - rows, 2 * latent), F32)], axis=0)
    total = total.T
    my_l[...] = pack(total[:latent] / jnp.sqrt(total[latent:] + 1.0), rows)
    out_l = []
    for d in range(1, n):
        out_l.append(
            remote(
                my_l, their_l.at[cell], ol_send.at[d - 1], ol_recv.at[d - 1],
                {"cell": lax.rem(cell + d, n)},
            )
        )
        out_l[-1].start()
    their_l[cell] = my_l[...]
    other_genes(1)
    other_genes(2)
    for z in others:
        remote(cl_own, cl_all.at[z], ca_send.at[0], ca_recv.at[z], {"gene": near}).wait_recv()
    for o in range(m):
        at = slice(o * span, (o + 1) * span)
        fs_ref[:, at] = (cl_all[o] - gf[:latent, at]) / (gf[latent:, at] + 1.0)
    for d in range(1, n):
        out_l[d - 1].wait()
    for o in range(n):
        unpack(ls_ref, o, rows, their_l.at[o])
    for copy in ca_line:
        copy.wait_send()


def pass_on(*refs):
    count = len(refs) // 2
    for source, target in zip(refs[:count], refs[count:]):
        target[...] = source[...]


def local_fused(
    n, m, counts, batch_id, live_cells, knot_bin, depth_frac, cell_covariates, coefficients,
    batch_effect, factors, loadings,
):
    genes, slots = counts.shape
    rows, span, latent = genes // n, slots // m, factors.shape[1]
    ncov = cell_covariates.shape[0]
    width = SPL + ncov
    wide = SPL * ncov + ncov * ncov * 3 // 4 + 2 * SPL + width
    chips = n // 2
    dma = pltpu.SemaphoreType.DMA
    shape = jax.ShapeDtypeStruct
    vmem = pltpu.VMEM

    def params(**kw):
        return pltpu.CompilerParams(vmem_limit_bytes=LIMIT, **kw)

    def stay(x):
        return pltpu.with_memory_space_constraint(x, pltpu.HBM)

    knot, frac, batch = (v.reshape(1, slots) for v in (knot_bin, depth_frac, batch_id))
    shapes = (shape((width, genes), F32), shape((latent, slots), F32), shape((latent, genes), F32))
    there = pl.BlockSpec(memory_space=pl.ANY)
    found = pl.pallas_call(
        functools.partial(all_kernel, n, m),
        out_shape=shapes,
        in_specs=[there, there, pl.BlockSpec(memory_space=pltpu.SMEM)] + [there] * 7,
        out_specs=(VM, VM, VM),
        scratch_shapes=[
            vmem((1, slots), jnp.int32),
            vmem((1, slots), jnp.int32),
            vmem((1, slots), F32),
            vmem((ncov, slots), F32),
            vmem((latent, slots), BF16),
            vmem((latent, genes), BF16),
            vmem((width + BATCHES + latent, genes), F32),
            vmem((m, width + BATCHES + latent, genes), F32),
            vmem((genes, slots), jnp.int32),
            vmem((genes, slots), F32),
            vmem((3 * width + 2 * BATCHES + latent, slots), BF16),
            vmem((wide, slots), BF16),
            vmem((wide, slots), BF16),
            vmem((2 * width + latent, slots), BF16),
            vmem((3 * latent, slots), BF16),
            vmem((3 * latent, genes), BF16),
            vmem((8, slots), F32),
            vmem((1, slots), F32),
            vmem((m - 1, 1, slots), F32),
            vmem((genes, 2 * width + latent), F32),
            vmem((latent, slots), F32),
            vmem((2, latent, span), F32),
            vmem((2, latent, span), F32),
            vmem((2, latent, span), F32),
            vmem((latent, span), F32),
            vmem((m, latent, span), F32),
            vmem((genes, slots), BF16),
            vmem((genes, slots), BF16),
            vmem((genes, 3 * width), BF16),
            vmem((chips, 2, rows, wide), F32),
            vmem((chips, rows, wide), F32),
            vmem((chips - 1, rows, wide), F32),
            vmem((2, rows // 2, wide), F32),
            vmem((2, rows, wide), F32),
            vmem((128, wide), F32),
            vmem((wide, 128), F32),
            vmem((width, 128), F32),
            vmem((width * rows // 128, 128), F32),
            vmem((m, 2, chips, width * rows // 128, 128), F32),
            vmem((width, genes), F32),
            vmem((chips, 2, rows, 2 * latent), F32),
            vmem((chips, rows, 2 * latent), F32),
            vmem((chips - 1, rows, 2 * latent), F32),
            vmem((chips - 1, rows, 2 * latent), F32),
            vmem((latent * rows // 128, 128), F32),
            vmem((n, latent * rows // 128, 128), F32),
            vmem((2 * latent, slots), F32),
            dma((n,)), dma((8,)), dma((m - 1,)), dma((m - 1,)),
            dma((m - 1,)), dma((m - 1,)), dma((2,)), dma((2,)),
            dma((m - 1,)), dma((m - 1,)),
            dma((chips,)), dma((chips,)), dma((2,)), dma((2,)), dma((4,)), dma((4,)),
            dma((m - 1,)), dma((m,)), dma((m - 1,)), dma((m,)),
            dma((n - 1,)), dma((n - 1,)), dma((m - 1,)), dma((m - 1,)),
            dma((m - 1, chips - 1)), dma((m - 1, chips - 1)), dma((m - 1,)), dma((m - 1,)),
            dma((chips,)), dma((chips,)), dma((chips - 1,)), dma((chips - 1,)),
            dma((n - 1,)), dma((n - 1,)),
        ],
        compiler_params=params(collective_id=0, has_side_effects=True),
        name="step",
    )(
        stay(counts), stay(batch), live_cells, stay(knot), stay(frac), stay(cell_covariates),
        stay(coefficients.T), stay(batch_effect.T), stay(factors.T), stay(loadings.T),
    )
    beta, fs, ls = pl.pallas_call(
        pass_on, out_shape=shapes, in_specs=[VM] * 3, out_specs=(VM, VM, VM),
        compiler_params=params(), name="finish",
    )(*found)
    return beta.T, fs.T, ls.T


def local(n, m, *args):
    counts, cov, factors = args[0], args[5], args[8]
    genes, slots = counts.shape
    fits = (
        n == 8
        and m == 4
        and genes % (16 * n) == 0
        and genes // n == 96
        and slots % (128 * m) == 0
        and genes % 256 == 0
        and (SPL + cov.shape[0] + BATCHES + factors.shape[1]) % 16 == 0
        and cov.shape[0] == SPL
        and factors.shape[1] == 64
    )
    if fits:
        return local_fused(n, m, *args)
    return local_plain(*args)


def solution(mesh):
    placed = (
        P("gene", "cell"),
        P("cell"),
        P("cell"),
        P("cell"),
        P("cell"),
        P(None, "cell"),
        P("gene", None),
        P("gene", None),
        P("cell", None),
        P("gene", None),
    )
    return jax.shard_map(
        functools.partial(local, mesh.shape["cell"], mesh.shape["gene"]),
        mesh=mesh,
        in_specs=placed,
        out_specs=(P("gene", None), P("cell", None), P("gene", None)),
        check_vma=False,
    )
```
